32 devices in a mesh: dom: 8 (over z, x), sub: 4 (over y, core).
Axes of the slice: x: 2, y: 2, z: 4, core: 2. Of those that a mesh axis runs over, the one named last changes fastest.
Arguments:
- primitive: float32 [5, 65536], P(None, ('dom', 'sub')), may hold values from -3 to 3
- gradient: float32 [15, 65536], P(None, ('dom', 'sub')), may hold values from -1.5 to 1.5
- volume: float32 [65536], P(('dom', 'sub')), may hold values from 0.5 to 4
- face_left: int32 [196608], P(('dom', 'sub')), may hold values from 0 to 2047
- face_right: int32 [196608], P(('dom', 'sub')), may hold values from 0 to 4095, as said below
- face_angles: float32 [2, 196608], P(None, ('dom', 'sub')), may hold values from -3.140625 to 3.140625
- face_area: float32 [196608], P(('dom', 'sub')), may hold values from 0.2 to 2
- face_offsets: float32 [6, 196608], P(None, ('dom', 'sub')), may hold values from -1 to 1
- rim_left: int32 [16384], P(('dom', 'sub')), may hold values from 0 to 511
- rim_right: int32 [16384], P(('dom', 'sub')), may hold values from 0 to 511
- rim_angles: float32 [2, 16384], P(None, ('dom', 'sub')), may hold values from -3.140625 to 3.140625
- rim_area: float32 [16384], P(('dom', 'sub')), may hold values from 0.2 to 2
- rim_offsets: float32 [6, 16384], P(None, ('dom', 'sub')), may hold values from -1 to 1
- send_list: int32 [512], P(('dom', 'sub')), may hold values from -1 to 15, as said below
Outputs:
- change_rate: float32 [5, 65536], P(None, ('dom', 'sub'))
- new_conserved: float32 [5, 65536], P(None, ('dom', 'sub'))
- time_step: float32 [], replicated
The draws below stay inside these ranges and needn't reach their ends.
Inputs may be any that keep to these rules, and one draw needn't show every extreme that they name: `send_list`: an entry is a block number of the sending device or -1 for an unused slot; for each peer the used slots come first, at most 4 of them, a device sends no block to itself, and each device fills all 4 slots of one peer. `face_right`: an entry of at least 2048 names ghost cell (s * 4 + j) * 128 + k only where slot j of the sending peer s is used.
All inputs are finite; a program needn't handle non-finite values.
Results may differ from the reference program's by a relative error of at most 0.0003.
Values sent between devices are 32-bit elements; how exact they have to be, the bound alone decides.
A program may use at most 64 MiB of HBM per device.

```python
import math
import jax
import jax.numpy as jnp
from jax import lax

BLK = 128
NB = 16
RIM = 4
CAP = 4
FACES = 6144
NCELL = 65536
NFACE = 196608
NRIM = 16384
N_DOM = 8
N_SUB = 4
DEVICES = 32


def peer_counts(key):
    key_counts = jax.random.fold_in(key, 11)
    base_counts = jax.random.randint(key_counts, (DEVICES, N_SUB), 1, CAP + 1)
    source = jnp.arange(DEVICES, dtype=jnp.int32) % N_SUB
    target = jnp.arange(N_SUB, dtype=jnp.int32)
    full_peer = target[None, :] == (source[:, None] + 1) % N_SUB
    counts = jnp.where(full_peer, CAP, base_counts)
    return jnp.where(target[None, :] == source[:, None], 0, counts).astype(jnp.int32)


def draw_send_list(key, part):
    counts = peer_counts(key)
    block_ids = jax.random.randint(jax.random.fold_in(key, 12), (DEVICES, N_SUB, CAP), 0, NB)
    slot_index = jnp.arange(CAP, dtype=jnp.int32)
    chosen = jnp.where(slot_index[None, None, :] < counts[:, :, None], block_ids, -1)
    return chosen.reshape(-1).astype(jnp.int32)


def draw_face_right(key, part):
    counts = peer_counts(key)
    device = jnp.arange(DEVICES, dtype=jnp.int32)[:, None]
    dom_index = device // N_SUB
    sub_index = device % N_SUB
    local_pick = jax.random.randint(jax.random.fold_in(key, 21), (DEVICES, FACES), 0, NB * BLK)
    source = jax.random.randint(jax.random.fold_in(key, 22), (DEVICES, FACES), 0, N_SUB)
    available = counts[dom_index * N_SUB + source, sub_index]
    slot_index = jax.random.randint(jax.random.fold_in(key, 23), (DEVICES, FACES), 0, CAP) % jnp.maximum(available, 1)
    cell_index = jax.random.randint(jax.random.fold_in(key, 24), (DEVICES, FACES), 0, BLK)
    coin_flip = jax.random.randint(jax.random.fold_in(key, 25), (DEVICES, FACES), 0, 4)
    ghost_pick = NB * BLK + (source * CAP + slot_index) * BLK + cell_index
    chosen = jnp.where((coin_flip == 0) & (available > 0), ghost_pick, local_pick)
    return chosen.reshape(-1).astype(jnp.int32)


def set_ends(array, rng, smallest, largest):
    spot = [jax.random.randint(jax.random.fold_in(rng, axis), (), 0, length) for axis, length in enumerate(array.shape)]
    longest = array.shape.index(max(array.shape))
    next_to = spot[:longest] + [(spot[longest] + 1) % array.shape[longest]] + spot[longest + 1:]
    return array.at[tuple(spot)].set(smallest).at[tuple(next_to)].set(largest)


def levels(key, extent, shards, least, largest):
    def one(axis_at, blocks):
        draws = jax.random.uniform(jax.random.fold_in(jax.random.fold_in(key, 6), axis_at), (blocks,), jnp.float32, least / len(shards), largest / len(shards))
        return jnp.repeat(jnp.exp(draws), extent[axis_at] // blocks).reshape((-1,) + (1,) * (len(extent) - axis_at - 1))

    factor_of = one(*shards[0])
    for cut in shards[1:]:
        factor_of = factor_of * one(*cut)
    return factor_of


def centred(own_key, dims, scale, limit, pieces=(), kind=jnp.bfloat16):
    result = jax.random.normal(own_key, dims, jnp.float32) * scale
    if len(pieces) > 0:
        result = levels(own_key, dims, pieces, -0.22, 0.18) * result
    return jnp.clip(result, min=-limit, max=limit).astype(kind)


def setup_inputs(seed: int = 0) -> dict:
    keys = jax.random.split(jax.random.key(seed), 15)
    return {
        "primitive": centred(keys[0], (5, NCELL), 0.5, 3.0, ((1, 32),), jnp.float32),
        "gradient": centred(keys[1], (15, NCELL), 0.3, 1.5, ((1, 32),), jnp.float32),
        "volume": jnp.clip(jnp.exp(math.log(4.0) - 2.0794415 * jax.random.uniform(keys[2], (NCELL,), jnp.float32) ** levels(keys[2], (NCELL,), ((0, 32),), -0.2, 0.2)), 0.5, 4.0),
        "face_left": set_ends(jax.random.randint(keys[3], (NFACE,), 0, NB * BLK), jax.random.fold_in(keys[3], 1), 0, (NB * BLK) - 1).astype(jnp.int32),
        "face_right": draw_face_right(jax.random.fold_in(keys[14], 71), 0),
        "face_angles": jnp.clip(jax.random.uniform(keys[5], (2, NFACE), jnp.float32, -3.140625, 3.140625), -3.140625, 3.140625),
        "face_area": jnp.clip(jnp.exp(math.log(2.0) - 2.3025851 * jax.random.uniform(keys[6], (NFACE,), jnp.float32) ** levels(keys[6], (NFACE,), ((0, 32),), -0.2, 0.2)), 0.2, 2.0),
        "face_offsets": centred(keys[7], (6, NFACE), 0.3, 1.0, ((1, 32),), jnp.float32),
        "rim_left": set_ends(jax.random.randint(keys[8], (NRIM,), 0, RIM * BLK), jax.random.fold_in(keys[8], 1), 0, (RIM * BLK) - 1).astype(jnp.int32),
        "rim_right": set_ends(jax.random.randint(keys[9], (NRIM,), 0, RIM * BLK), jax.random.fold_in(keys[9], 1), 0, (RIM * BLK) - 1).astype(jnp.int32),
        "rim_angles": jnp.clip(jax.random.uniform(keys[10], (2, NRIM), jnp.float32, -3.140625, 3.140625), -3.140625, 3.140625),
        "rim_area": jnp.clip(jnp.exp(math.log(2.0) - 2.3025851 * jax.random.uniform(keys[11], (NRIM,), jnp.float32) ** levels(keys[11], (NRIM,), ((0, 32),), -0.2, 0.2)), 0.2, 2.0),
        "rim_offsets": centred(keys[12], (6, NRIM), 0.3, 1.0, ((1, 32),), jnp.float32),
        "send_list": draw_send_list(jax.random.fold_in(keys[14], 71), 0),
    }


adiabatic = 5.0 / 3.0
courant = 0.3

def face_states(side_cells, shifts):
    centre_values = side_cells[:5]
    slopes = side_cells[5:].reshape(5, 3, -1)
    values = centre_values + lax.optimization_barrier(jnp.sum(slopes * shifts[None], axis=1))
    return (jnp.exp(values[0]), values[1:4], jnp.exp(values[4]))

def conserved_flux(density, velocity, pressure, normal):
    normal_speed = lax.optimization_barrier(jnp.sum(velocity * normal, axis=0))
    energy = pressure / (adiabatic - 1.0) + 0.5 * density * lax.optimization_barrier(jnp.sum(velocity * velocity, axis=0))
    conserved = jnp.concatenate([density[None], density * velocity, energy[None]], 0)
    flux_vector = jnp.concatenate([(density * normal_speed)[None], density * velocity * normal_speed + pressure * normal, ((energy + pressure) * normal_speed)[None]], 0)
    return (normal_speed, energy, conserved, flux_vector)

def star_flux(density, velocity, pressure, normal, normal_speed, energy, conserved, flux_vector, signal, contact):
    mass_rate = density * (signal - normal_speed)
    factor = mass_rate / (signal - contact)
    star_state = factor * jnp.concatenate([jnp.ones_like(density)[None], velocity + (contact - normal_speed) * normal, (energy / density + (contact - normal_speed) * (contact + pressure / mass_rate))[None]], 0)
    return flux_vector + signal * (star_state - conserved)

def hllc_flux(left_cells, right_cells, angles, offsets):
    normal = jnp.stack([jnp.sin(angles[0]) * jnp.cos(angles[1]), jnp.sin(angles[0]) * jnp.sin(angles[1]), jnp.cos(angles[0])], 0)
    density_left, velocity_left, pressure_left = face_states(left_cells, offsets[0:3])
    density_right, velocity_right, pressure_right = face_states(right_cells, offsets[3:6])
    speed_left, energy_left, state_left, flux_left = conserved_flux(density_left, velocity_left, pressure_left, normal)
    speed_right, energy_right, state_right, flux_right = conserved_flux(density_right, velocity_right, pressure_right, normal)
    sound_left = jnp.sqrt(adiabatic * pressure_left / density_left)
    sound_right = jnp.sqrt(adiabatic * pressure_right / density_right)
    signal_left = jnp.minimum(speed_left - sound_left, speed_right - sound_right)
    signal_right = jnp.maximum(speed_left + sound_left, speed_right + sound_right)
    mass_left = density_left * (signal_left - speed_left)
    mass_right = density_right * (signal_right - speed_right)
    contact = (pressure_right - pressure_left + mass_left * speed_left - mass_right * speed_right) / (mass_left - mass_right)
    star_left = star_flux(density_left, velocity_left, pressure_left, normal, speed_left, energy_left, state_left, flux_left, signal_left, contact)
    star_right = star_flux(density_right, velocity_right, pressure_right, normal, speed_right, energy_right, state_right, flux_right, signal_right, contact)
    return jnp.where(signal_left >= 0, flux_left, jnp.where(contact >= 0, star_left, jnp.where(signal_right > 0, star_right, flux_right)))

def cell_conserved(primitive):
    density = jnp.exp(primitive[0])
    pressure = jnp.exp(primitive[4])
    velocity = primitive[1:4]
    energy = pressure / (adiabatic - 1.0) + 0.5 * density * lax.optimization_barrier(jnp.sum(velocity * velocity, axis=0))
    return jnp.concatenate([density[None], density * velocity, energy[None]], 0)

def signal_limit(primitive, volume):
    density = jnp.exp(primitive[0])
    pressure = jnp.exp(primitive[4])
    velocity = primitive[1:4]
    sound_speed = jnp.sqrt(adiabatic * pressure / density)
    flow_speed = jnp.sqrt(lax.optimization_barrier(jnp.sum(velocity * velocity, axis=0)))
    return volume ** (1.0 / 3.0) / (sound_speed + flow_speed)

def reference(primitive, gradient, volume, face_left, face_right, face_angles, face_area, face_offsets, rim_left, rim_right, rim_angles, rim_area, rim_offsets, send_list):
    devices = N_DOM * N_SUB
    local_cells = NB * BLK
    ghost_cells = N_SUB * CAP * BLK
    rim_width = RIM * BLK
    rim_faces = RIM * BLK
    packed = jnp.concatenate([primitive, gradient], 0)
    blocks = packed.reshape(20, devices * NB, BLK)
    wanted = send_list.reshape(N_DOM, N_SUB, N_SUB, CAP)
    owner = (jnp.arange(N_DOM, dtype=jnp.int32)[:, None, None, None] * N_SUB + jnp.arange(N_SUB, dtype=jnp.int32)[None, :, None, None]) * NB
    global_ids = jnp.transpose(owner + jnp.maximum(wanted, 0), (0, 2, 1, 3)).reshape(-1).astype(jnp.int32)
    in_use = jnp.transpose(wanted >= 0, (0, 2, 1, 3)).reshape(-1)
    ghosts = jnp.take(blocks, global_ids, axis=1) * in_use.astype(jnp.float32)[None, :, None]
    ghosts = ghosts.reshape(20, devices, ghost_cells)
    segments = packed.reshape(20, N_DOM, N_SUB, local_cells)
    following = jnp.concatenate([segments[:, 1:, :, :rim_width], jnp.zeros((20, 1, N_SUB, rim_width), jnp.float32)], 1).reshape(20, devices, rim_width)
    local_view = packed.reshape(20, devices, local_cells)

    def one_device(device):
        own_cells = lax.dynamic_index_in_dim(local_view, device, 1, keepdims=False)
        own_ghosts = lax.dynamic_index_in_dim(ghosts, device, 1, keepdims=False)
        next_cells = lax.dynamic_index_in_dim(following, device, 1, keepdims=False)
        left_index = lax.dynamic_slice_in_dim(face_left, device * FACES, FACES)
        right_index = lax.dynamic_slice_in_dim(face_right, device * FACES, FACES)
        angles = lax.dynamic_slice_in_dim(face_angles, device * FACES, FACES, 1)
        areas = lax.dynamic_slice_in_dim(face_area, device * FACES, FACES)
        offsets = lax.dynamic_slice_in_dim(face_offsets, device * FACES, FACES, 1)
        combined = jnp.concatenate([own_cells, own_ghosts], 1)
        weighted = hllc_flux(jnp.take(own_cells, left_index, axis=1), jnp.take(combined, right_index, axis=1), angles, offsets) * areas
        totals = jnp.zeros((5, local_cells + ghost_cells), jnp.float32).at[:, left_index].add(weighted).at[:, right_index].add(-weighted)
        rim_lidx = lax.dynamic_slice_in_dim(rim_left, device * rim_faces, rim_faces)
        rim_ridx = lax.dynamic_slice_in_dim(rim_right, device * rim_faces, rim_faces)
        rim_ang = lax.dynamic_slice_in_dim(rim_angles, device * rim_faces, rim_faces, 1)
        rim_areas = lax.dynamic_slice_in_dim(rim_area, device * rim_faces, rim_faces)
        rim_offs = lax.dynamic_slice_in_dim(rim_offsets, device * rim_faces, rim_faces, 1)
        rim_mask = (device // N_SUB < N_DOM - 1).astype(jnp.float32)
        tail_cells = own_cells[:, local_cells - rim_width:]
        rim_flux = hllc_flux(jnp.take(tail_cells, rim_lidx, axis=1), jnp.take(next_cells, rim_ridx, axis=1), rim_ang, rim_offs) * (rim_areas * rim_mask)
        net_flux = totals[:, :local_cells].at[:, local_cells - rim_width + rim_lidx].add(rim_flux)
        rim_back = jnp.zeros((5, rim_width), jnp.float32).at[:, rim_ridx].add(-rim_flux)
        return (net_flux, totals[:, local_cells:], rim_back)
    net_parts, ghost_back, rim_back = lax.map(one_device, jnp.arange(devices, dtype=jnp.int32))
    ghost_back = jnp.transpose(ghost_back, (1, 0, 2)).reshape(5, devices * N_SUB * CAP, BLK)
    target = jnp.where(in_use, global_ids, devices * NB).astype(jnp.int32)
    returned = jnp.zeros((5, devices * NB, BLK), jnp.float32).at[:, target].add(ghost_back, mode='drop')
    net_flux = jnp.transpose(net_parts, (1, 0, 2)) + returned.reshape(5, devices, local_cells)
    rim_inflow = jnp.concatenate([jnp.zeros((N_SUB, 5, rim_width), jnp.float32), rim_back[:devices - N_SUB]], 0)
    net_flux = net_flux.at[:, :, :rim_width].add(jnp.transpose(rim_inflow, (1, 0, 2)))
    net_flux = net_flux.reshape(5, devices * local_cells)
    time_step = courant * jnp.min(signal_limit(primitive, volume))
    change_rate = -net_flux / volume
    new_conserved = cell_conserved(primitive) + time_step * change_rate
    return (change_rate, new_conserved, time_step)
```

```python
import functools
import jax
import jax.numpy as jnp
from jax import lax
from jax.experimental import pallas as pl
from jax.experimental.pallas import tpu as pltpu
from jax.sharding import PartitionSpec as P

BLK = 128
RIM = 4
GROUP = 13
PIECES = 2
RAW = 6
PACKED = 7
GRAD_MAX = 1.5
GRAD_STEPS = 32767.0

adiabatic = 5.0 / 3.0
courant = 0.3
MESH = pl.DeviceIdType.MESH


def sin_cos(x):
    turns = jnp.floor(x * 0.63661977236 + 0.5)
    r = (x - turns * 1.57079637050628662109375) - turns * -4.37113900018624283e-8
    r2 = r * r
    sine = r + r * r2 * (-1.6666667163e-1 + r2 * (8.3333337680e-3 + r2 * (-1.9841270114e-4 + r2 * 2.7557314297e-6)))
    cosine = 1.0 + r2 * (-0.5 + r2 * (4.1666667908e-2 + r2 * (-1.3888889225e-3 + r2 * 2.4801587642e-5)))
    odd = jnp.abs(turns) == 1.0
    s = jnp.where(odd, cosine, sine)
    c = jnp.where(odd, sine, cosine)
    s = jnp.where((turns < 0.0) | (turns > 1.0), -s, s)
    c = jnp.where((turns > 0.0) | (turns < -1.0), -c, c)
    return s, c


def pack_pair(a, b):
    scale = GRAD_STEPS / GRAD_MAX
    high = (a * scale + 32768.5).astype(jnp.int32)
    low = (b * scale + 32768.5).astype(jnp.int32)
    return lax.shift_left(high, jnp.full_like(high, 16)) + (low + jnp.int32(-(2**31)))


def gradients(raw, packed):
    out = [None] * 15
    for w in range(PACKED):
        word = packed(w)
        out[w] = lax.shift_right_arithmetic(word, jnp.full_like(word, 16)).astype(jnp.float32)
        out[w + 8] = ((word & 65535) - 32768).astype(jnp.float32)
    out[7] = raw(5) * (GRAD_STEPS / GRAD_MAX)
    return out


def side_state(raw, packed, offsets):
    step = GRAD_MAX / GRAD_STEPS
    offsets = [r * step for r in offsets]
    slope = gradients(raw, packed)
    values = [
        raw(c) + (slope[3 * c] * offsets[0] + slope[3 * c + 1] * offsets[1] + slope[3 * c + 2] * offsets[2])
        for c in range(5)
    ]
    sound = jnp.exp((values[4] - values[0]) * 0.5) * (adiabatic**0.5)
    return jnp.exp(values[0]), values[1:4], jnp.exp(values[4]), sound


def dot3(a, b):
    return a[0] * b[0] + a[1] * b[1] + a[2] * b[2]


def hllc(normal, left, right):
    dl, vl, pl_, cl, ul = left
    dr, vr, pr, cr = right
    ur = dot3(vr, normal)
    signal_l = jnp.minimum(ul - cl, ur - cr)
    signal_r = jnp.maximum(ul + cl, ur + cr)
    mass_l = dl * (signal_l - ul)
    mass_r = dr * (signal_r - ur)
    contact = (pr - pl_ + mass_l * ul - mass_r * ur) / (mass_l - mass_r)
    outer = signal_l >= 0
    from_left = jnp.logical_or(outer, contact >= 0)
    starred = jnp.where(from_left, signal_l, -signal_r) < 0
    pick = lambda a, b: jnp.where(from_left, a, b)
    density, pressure, speed, sound = pick(dl, dr), pick(pl_, pr), pick(ul, ur), pick(cl, cr)
    velocity = [pick(a, b) for a, b in zip(vl, vr)]
    signal, mass_rate = pick(signal_l, signal_r), pick(mass_l, mass_r)
    specific = sound * sound * (1.0 / (adiabatic * (adiabatic - 1.0))) + 0.5 * dot3(velocity, velocity)
    energy = density * specific
    jump = contact - speed
    factor = mass_rate / (signal - contact)
    rise = jnp.where(starred, signal * (factor - density), 0.0)
    push = jnp.where(starred, signal * factor * jump, 0.0)
    rate = density * speed
    out = [rate + rise]
    along = pressure + push
    carry = rate + rise
    for v, n in zip(velocity, normal):
        out.append(carry * v + along * n)
    out.append((energy + pressure) * speed + rise * specific + push * (contact + pressure / mass_rate))
    return out


def lane_gather(row, index):
    table = jnp.broadcast_to(row, index.shape)
    return jnp.take_along_axis(table, index, axis=1, mode="promise_in_bounds")


def flip(index, mask, size):
    out, bit = index, 1
    while bit < size:
        if mask & bit:
            out = out + bit * (1 - 2 * lax.rem(lax.div(index, bit), 2))
        bit *= 2
    return out


def kernel(
    dims,
    send_hbm,
    prim_rows,
    grad_hbm,
    volume_hbm,
    left_hbm,
    right_hbm,
    angles_hbm,
    area_hbm,
    offsets_hbm,
    rim_left_hbm,
    rim_right_hbm,
    rim_angles_hbm,
    rim_area_hbm,
    rim_offsets_hbm,
    rate_out,
    new_out,
    step_out,
    send_list,
    prim,
    cells,
    grad,
    volume,
    face_left,
    face_right,
    angles,
    area,
    offsets,
    rim_left,
    rim_right,
    outgoing,
    ghosts,
    next_prim,
    next_grad,
    own_packed,
    ghost_packed,
    next_packed,
    min_own,
    mins,
    min_spare,
    min_base,
    prefix_send,
    prefix_recv,
    gback_send,
    gback_recv,
    rback_send,
    rback_recv,
    hi_left,
    lo_left,
    hi_right,
    lo_right,
    left_raw,
    left_packed,
    right_raw,
    right_packed,
    ready,
    pieces,
    load_sem,
    ghost_send_sem,
    ghost_recv_sem,
    rim_send_sem,
    rim_recv_sem,
    min_send_sem,
    min_recv_sem,
    prefix_send_sem,
    prefix_recv_sem,
    gback_send_sem,
    gback_recv_sem,
    rback_send_sem,
    rback_recv_sem,
    hello_above,
    hello_next,
):
    n_dom, n_sub, capacity, blocks, face_rows = dims
    rows = face_rows + RIM
    group = max(k for k in range(1, GROUP + 1) if rows % k == 0)
    ghost_blocks = n_sub * capacity
    me_dom = lax.axis_index("dom")
    me_sub = lax.axis_index("sub")
    plane = 2 if n_dom % 2 == 0 else 1
    planes = n_dom // plane
    my_plane = lax.div(me_dom, plane)
    base_dom = my_plane * plane
    last = me_dom == n_dom - 1
    first = me_dom == 0
    power = n_sub & (n_sub - 1) == 0

    def to_peer(k):
        return flip(me_sub, k, n_sub) if power else lax.rem(me_sub + k, n_sub)

    def from_peer(k):
        return flip(me_sub, k, n_sub) if power else lax.rem(me_sub + n_sub - k, n_sub)

    far_first = list(range(n_sub - 1, 0, -1))

    tail = pl.ds(face_rows, RIM)
    pairs = [(send_hbm, send_list), (prim_rows, prim)]
    pairs += [(grad_hbm.at[:, h * BLK : (h + 1) * BLK], grad.at[h]) for h in range(blocks)]
    early = len(pairs)
    pairs += [(prim_rows.at[:, r, :], cells.at[r]) for r in range(5)]
    pairs += [(volume_hbm, volume)]
    middle = len(pairs)
    pairs += [(left_hbm, face_left), (right_hbm, face_right), (rim_left_hbm, rim_left), (rim_right_hbm, rim_right)]
    indices = len(pairs)
    pairs += [(angles_hbm.at[:, r, :], angles.at[r, 0:face_rows, :]) for r in range(2)]
    pairs += [(offsets_hbm.at[:, r, :], offsets.at[r, 0:face_rows, :]) for r in range(6)]
    pairs += [(area_hbm, area.at[0:face_rows, :])]
    pairs += [(rim_angles_hbm.at[:, r, :], angles.at[r, tail, :]) for r in range(2)]
    pairs += [(rim_offsets_hbm.at[:, r, :], offsets.at[r, tail, :]) for r in range(6)]
    pairs += [(rim_area_hbm, area.at[tail, :])]
    loads = [pltpu.make_async_copy(a, b, load_sem.at[k]) for k, (a, b) in enumerate(pairs)]
    for load in loads[:middle]:
        load.start()

    barrier = pltpu.get_barrier_semaphore()
    for step in range(plane):
        dom = base_dom + lax.rem(me_dom + step, plane)
        for k in range(n_sub):
            if step or k:
                pl.semaphore_signal(barrier, inc=1, device_id=(dom, to_peer(k)), device_id_type=MESH)

    def greet(p, carry):
        for step in range(plane):
            for k in range(n_sub):
                pl.semaphore_signal(barrier, inc=1, device_id=(p * plane + step, k), device_id_type=MESH)
        return carry

    for load in loads[middle:]:
        load.start()
    lax.fori_loop(my_plane + 1, planes, greet, 0)

    for load in loads[:early]:
        load.wait()
    for k in far_first:
        for j in range(capacity):
            block = jnp.maximum(send_list[to_peer(k) * capacity + j], 0)
            slopes, centres = grad[block], prim[block]
            outgoing[k, 8 * j : 8 * j + 8, :] = slopes[0:8]
            low = 8 * capacity + 8 * j
            outgoing[k, low : low + 7, :] = slopes[8:15]
            outgoing[k, low + 7 : low + 8, :] = centres[0:1]
            outgoing[k, 16 * capacity + 4 * j : 16 * capacity + 4 * j + 4, :] = centres[1:5]

    for load in loads[early:middle]:
        load.wait()
    signal = jnp.exp((cells[4] - cells[0]) * 0.5) * (adiabatic**0.5) + jnp.sqrt(
        cells[1] * cells[1] + cells[2] * cells[2] + cells[3] * cells[3]
    )
    limit = jnp.exp(jnp.log(volume[...]) * (1.0 / 3.0)) / signal
    min_own[...] = jnp.min(limit, axis=0, keepdims=True)

    for h in range(blocks):
        own_packed[h, 0:PACKED, :] = pack_pair(grad[h, 0:7, :], grad[h, 8:15, :])

    for load in loads[middle:indices]:
        load.wait()
    twice = lambda ref: jnp.concatenate([ref[...], ref[...]], 0)
    main = slice(0, face_rows)
    over = slice(face_rows, face_rows + 8)
    high = lambda x: lax.shift_right_logical(x, jnp.full_like(x, 7))
    hi_left[main, :] = high(face_left[...])
    lo_left[main, :] = face_left[...] & (BLK - 1)
    hi_right[main, :] = high(face_right[...])
    lo_right[main, :] = face_right[...] & (BLK - 1)
    hi_left[over, :] = high(twice(rim_left)) + (blocks - RIM)
    lo_left[over, :] = twice(rim_left) & (BLK - 1)
    hi_right[over, :] = high(twice(rim_right)) + (blocks + ghost_blocks)
    lo_right[over, :] = twice(rim_right) & (BLK - 1)

    count = plane * n_sub - 1 + plane * n_sub * my_plane
    pl.semaphore_wait(barrier, count)

    def remote(src, dst, send, recv, dom, sub):
        return pltpu.make_async_remote_copy(
            src_ref=src, dst_ref=dst, send_sem=send, recv_sem=recv, device_id=(dom, sub), device_id_type=MESH
        )

    def min_copy(dom, sub, p):
        return remote(min_own, mins.at[me_dom, me_sub], min_send_sem.at[p], min_recv_sem.at[my_plane], dom, sub)

    for step in range(plane):
        dom = base_dom + lax.rem(me_dom + step, plane)
        for k in range(n_sub):
            if step or k:
                min_copy(dom, to_peer(k), my_plane).start()

    ghost_copies = {
        k: remote(outgoing.at[k], ghosts.at[k], ghost_send_sem.at[k], ghost_recv_sem.at[k], me_dom, to_peer(k))
        for k in far_first
    }
    for k in far_first:
        ghost_copies[k].start()
    rim_copies = [
        remote(src.at[0:RIM], dst, rim_send_sem.at[i], rim_recv_sem.at[i], me_dom - 1, me_sub)
        for i, (src, dst) in enumerate([(prim, next_prim), (grad, next_grad)])
    ]

    def tell(p, carry):
        for step in range(plane):
            for k in range(n_sub):
                min_copy(p * plane + step, k, p).start()
        return carry

    @pl.when(jnp.logical_not(first))
    def _():
        for copy in rim_copies:
            copy.start()

    lax.fori_loop(0, my_plane, tell, 0)

    @pl.when(my_plane > 0)
    def _():
        pl.semaphore_signal(hello_above, inc=1, device_id=(me_dom - plane, me_sub), device_id_type=MESH)

    @pl.when(jnp.logical_and(lax.rem(me_dom, plane) == 0, me_dom > 0))
    def _():
        pl.semaphore_signal(hello_next, inc=1, device_id=(me_dom - 1, me_sub), device_id_type=MESH)

    def own_row(h):
        def row(c):
            if c < 5:
                return cells[c, h : h + 1, :]
            if c == 5:
                return grad[h, 7:8, :]
            return own_packed[h, c - RAW : c - RAW + 1, :]

        return row

    def ghost_row(k, j):
        def row(c):
            if c == 0:
                at = 8 * capacity + 8 * j + 7
            elif c < 5:
                at = 16 * capacity + 4 * j + c - 1
            elif c == 5:
                at = 8 * j + 7
            else:
                return ghost_packed[k, j, c - RAW : c - RAW + 1, :]
            return ghosts[k, at : at + 1, :]

        return row

    def next_row(h):
        def row(c):
            if c < 5:
                return next_prim[h, c : c + 1, :]
            if c == 5:
                return next_grad[h, 7:8, :]
            return next_packed[h, c - RAW : c - RAW + 1, :]

        return row

    def gather_into(raw, packed, hi, lo, starts, sources, names, keep):
        at = [pl.ds(s, 8) for s in starts]
        index = [lo[here, :] for here in at]
        wanted = [hi[here, :] for here in at]
        match = [[w == name for name in names] for w in wanted]
        for c in range(RAW + PACKED):
            target, place = (raw, c) if c < RAW else (packed, c - RAW)
            values = [target[place, here, :] for here in at] if keep else [None] * len(at)
            for n, row in enumerate(sources):
                line = row(c)
                for i in range(len(at)):
                    got = lane_gather(line, index[i])
                    values[i] = got if values[i] is None else jnp.where(match[i][n], got, values[i])
            for here, value in zip(at, values):
                target[place, here, :] = value

    def gather_main(raw, packed, hi, lo, sources, names, keep, width):
        while (face_rows // 8) % width:
            width -= 1

        def one(g, carry):
            starts = [pl.multiple_of(g * (8 * width) + 8 * i, 8) for i in range(width)]
            gather_into(raw, packed, hi, lo, starts, sources, names, keep)
            return carry

        lax.fori_loop(0, face_rows // (8 * width), one, 0)

    own = [own_row(h) for h in range(blocks)]
    gather_main(left_raw, left_packed, hi_left, lo_left, own, range(blocks), False, 2)
    gather_into(
        left_raw, left_packed, hi_left, lo_left, [face_rows], own[blocks - RIM :], range(blocks - RIM, blocks), False
    )
    gather_main(right_raw, right_packed, hi_right, lo_right, own, range(blocks), False, 2)

    for load in loads[indices:]:
        load.wait()
    for r in range(2):
        angles[r, face_rows + RIM : face_rows + 8, :] = angles[r, tail, :]
    for r in range(6):
        offsets[r, face_rows + RIM : face_rows + 8, :] = offsets[r, tail, :]
    area[face_rows + RIM : face_rows + 8, :] = area[tail, :]

    def left_step(g, carry):
        here = pl.ds(pl.multiple_of(g * 8, 8), 8)
        sin_a, cos_a = sin_cos(angles[0, here, :])
        sin_b, cos_b = sin_cos(angles[1, here, :])
        normal = [sin_a * cos_b, sin_a * sin_b, cos_a]
        density, velocity, pressure, sound = side_state(
            lambda c: left_raw[c, here, :],
            lambda w: left_packed[w, here, :],
            [offsets[k, here, :] for k in range(3)],
        )
        values = normal + [density] + velocity + [pressure, sound, dot3(velocity, normal)]
        for k, value in enumerate(values):
            ready[k, here, :] = value
        return carry

    lax.fori_loop(0, (face_rows + 8) // 8, left_step, 0)

    def await_mins(semaphore, count):
        some = min_spare.at[0:count]
        pltpu.make_async_copy(some, some, semaphore).wait()

    def own_plane_min():
        await_mins(min_recv_sem.at[my_plane], plane * n_sub - 1)
        small = min_own[...]
        for step in range(1, plane * n_sub):
            dom = base_dom + lax.rem(me_dom + step // n_sub, plane)
            sub = lax.rem(me_sub + step, n_sub)
            small = jnp.minimum(small, mins[dom, sub])
        min_base[...] = small

        @pl.when(my_plane > 0)
        def _():
            prefix_copy.wait_recv()
            min_base[...] = jnp.minimum(min_base[...], prefix_recv[...])

    prefix_copy = remote(prefix_send, prefix_recv, prefix_send_sem, prefix_recv_sem, me_dom + plane, me_sub)

    def pass_on(mine):
        @pl.when(mine)
        def _():
            own_plane_min()
            prefix_send[...] = min_base[...]
            pl.semaphore_wait(hello_above, 1)
            prefix_copy.start()

    not_top = my_plane < planes - 1
    pass_on(jnp.logical_and(not_top, my_plane == 0))

    def pack_ghosts(k):
        for j in range(capacity):
            low = 8 * capacity + 8 * j
            ghost_packed[k, j, 0:PACKED, :] = pack_pair(ghosts[k, 8 * j : 8 * j + 7, :], ghosts[k, low : low + 7, :])

    def ghost_pass(ks):
        for k in ks:
            ghost_copies[k].wait()
            pack_ghosts(k)
        sources = [ghost_row(k, j) for k in ks for j in range(capacity)]
        names = [blocks + from_peer(k) * capacity + j for k in ks for j in range(capacity)]
        gather_main(right_raw, right_packed, hi_right, lo_right, sources, names, True, 3)

    ghost_pass([1])

    @pl.when(last)
    def _():
        next_prim[...] = jnp.zeros_like(next_prim)
        next_grad[...] = jnp.zeros_like(next_grad)

    @pl.when(jnp.logical_not(last))
    def _():
        for copy in rim_copies:
            copy.wait_recv()

    for h in range(RIM):
        next_packed[h, 0:PACKED, :] = pack_pair(next_grad[h, 0:7, :], next_grad[h, 8:15, :])
    start = blocks + ghost_blocks
    gather_into(
        right_raw,
        right_packed,
        hi_right,
        lo_right,
        [face_rows],
        [next_row(h) for h in range(RIM)],
        range(start, start + RIM),
        False,
    )

    ghost_pass([k for k in far_first if k > 1])
    pass_on(jnp.logical_and(not_top, lax.rem(my_plane, 2) == 1))

    def flux_step(g, carry):
        here = pl.ds(pl.multiple_of(g * 8, 8), 8)
        kept = [ready[k, here, :] for k in range(10)]
        right = side_state(
            lambda c: right_raw[c, here, :],
            lambda w: right_packed[w, here, :],
            [offsets[k, here, :] for k in range(3, 6)],
        )
        flux = hllc(kept[:3], (kept[3], kept[4:7], kept[7], kept[8], kept[9]), right)
        idle = jnp.logical_and(g * 8 >= face_rows, last)
        for c in range(5):
            value = jnp.where(idle, 0.0, flux[c] * area[here, :])
            big = value.astype(jnp.bfloat16).astype(jnp.float32)
            pieces[c, here, :] = big
            pieces[5 + c, here, :] = value - big
        return carry

    lax.fori_loop(0, (face_rows + 8) // 8, flux_step, 0)
    pass_on(functools.reduce(jnp.logical_and, [not_top, lax.rem(my_plane, 2) == 0, my_plane > 0]))

    lane_iota = lax.broadcasted_iota(jnp.int32, (BLK, BLK), 0)

    def one_hot(lo, s):
        return jnp.where(lane_iota == lo[pl.ds(s, 1), :], 1.0, 0.0).astype(jnp.bfloat16)

    def spread(hi, s, place, sign):
        match = place == hi[pl.ds(s, 1), :]
        parts = []
        for c in range(5 * PIECES):
            value = pieces[c, pl.ds(s, 1), :]
            value = value if sign > 0 else -value
            parts.append(jnp.where(match, value, 0.0))
        return jnp.concatenate(parts, 0).astype(jnp.bfloat16)

    def product(a, b):
        return lax.dot_general(a, b, (((1,), (1,)), ((), ())), preferred_element_type=jnp.float32)

    def fold(total, count):
        total = total.reshape(PIECES, 5, count, BLK)
        return total[0] + total[1]

    sent = (n_sub - 1) * capacity
    away = -(-(sent + RIM) // 8) * 8
    spot = lax.broadcasted_iota(jnp.int32, (away, BLK), 0)
    away_place = spot - sent + (blocks + ghost_blocks)
    for k in range(1, n_sub):
        lower = (k - 1) * capacity
        away_place = jnp.where(
            (spot >= lower) & (spot < lower + capacity), spot - lower + (blocks + from_peer(k) * capacity), away_place
        )
    own_place = lax.broadcasted_iota(jnp.int32, (blocks, BLK), 0)

    def away_step(i, total):
        a = jnp.concatenate([spread(hi_right, i * group + k, away_place, -1) for k in range(group)], 1)
        b = jnp.concatenate([one_hot(lo_right, i * group + k) for k in range(group)], 1)
        return total + product(a, b)

    total = lax.fori_loop(0, rows // group, away_step, jnp.zeros((5 * PIECES * away, BLK), jnp.float32))
    total = fold(total, away)
    for k in range(1, n_sub):
        gback_send[k] = total[:, (k - 1) * capacity : k * capacity, :]
    rback_send[...] = total[:, sent : sent + RIM, :]
    gback_copies = {
        k: remote(
            gback_send.at[k], gback_recv.at[k], gback_send_sem.at[k], gback_recv_sem.at[k], me_dom, from_peer(k)
        )
        for k in far_first
    }
    for k in far_first:
        gback_copies[k].start()
    rback_copy = remote(rback_send, rback_recv, rback_send_sem, rback_recv_sem, me_dom + 1, me_sub)

    @pl.when(jnp.logical_and(lax.rem(me_dom, plane) == plane - 1, jnp.logical_not(last)))
    def _():
        pl.semaphore_wait(hello_next, 1)

    @pl.when(jnp.logical_not(last))
    def _():
        rback_copy.start()

    def local_step(i, total):
        a = [spread(hi_left, i * group + k, own_place, 1) for k in range(group)]
        a += [spread(hi_right, i * group + k, own_place, -1) for k in range(group)]
        b = [one_hot(lo_left, i * group + k) for k in range(group)]
        b += [one_hot(lo_right, i * group + k) for k in range(group)]
        return total + product(jnp.concatenate(a, 1), jnp.concatenate(b, 1))

    total = lax.fori_loop(0, rows // group, local_step, jnp.zeros((5 * PIECES * blocks, BLK), jnp.float32))
    net = fold(total, blocks)

    @pl.when(jnp.logical_not(not_top))
    def _():
        own_plane_min()

    def later(p, small):
        await_mins(min_recv_sem.at[p], plane * n_sub)
        for step in range(plane):
            for k in range(n_sub):
                small = jnp.minimum(small, mins[p * plane + step, k])
        return small

    smallest = lax.fori_loop(my_plane + 1, planes, later, min_base[...])
    time_step = courant * jnp.min(smallest, axis=1, keepdims=True)
    step_out[0] = courant * jnp.min(smallest)

    @pl.when(first)
    def _():
        rback_recv[...] = jnp.zeros_like(rback_recv)

    @pl.when(jnp.logical_not(first))
    def _():
        rback_copy.wait_recv()

    for k in far_first:
        gback_copies[k].wait()

    square = cells[1] * cells[1] + cells[2] * cells[2] + cells[3] * cells[3]
    density = jnp.exp(cells[0])
    energy = jnp.exp(cells[4]) / (adiabatic - 1.0) + 0.5 * density * square
    conserved = [density, density * cells[1], density * cells[2], density * cells[3], energy]
    inverse = -1.0 / volume[...]
    for c in range(5):
        sums = net[c]
        for h in range(RIM):
            sums = sums + jnp.where(own_place == h, rback_recv[c, h : h + 1, :], 0.0)
        for k in range(1, n_sub):
            for j in range(capacity):
                wanted = send_list[to_peer(k) * capacity + j]
                sums = sums + jnp.where(own_place == wanted, gback_recv[k, c, j : j + 1, :], 0.0)
        rate = sums * inverse
        new = conserved[c] + time_step * rate
        rate_out[:, c, :] = rate
        new_out[:, c, :] = new

    @pl.when(jnp.logical_not(first))
    def _():
        for copy in rim_copies:
            copy.wait_send()

    @pl.when(jnp.logical_not(last))
    def _():
        rback_copy.wait_send()

    @pl.when(not_top)
    def _():
        prefix_copy.wait_send()

    await_mins(min_send_sem.at[my_plane], plane * n_sub - 1)

    def told(p, carry):
        await_mins(min_send_sem.at[p], plane * n_sub)
        return carry

    lax.fori_loop(0, my_plane, told, 0)


def finish(rate, new, step, rate_out, new_out, step_out, sems):
    pairs = ((rate, rate_out), (new, new_out), (step, step_out))
    copies = [pltpu.make_async_copy(a, b, sems.at[k]) for k, (a, b) in enumerate(pairs)]
    for copy in copies:
        copy.start()
    for copy in copies:
        copy.wait()


def by_block(x):
    return x.reshape(x.shape[0], x.shape[1] // BLK, BLK).transpose(1, 0, 2)


def body(mesh_sizes, *args):
    (primitive, gradient, volume, face_left, face_right, face_angles, face_area, face_offsets) = args[:8]
    (rim_left, rim_right, rim_angles, rim_area, rim_offsets, send_list) = args[8:]
    n_dom, n_sub = mesh_sizes
    cells = primitive.shape[1]
    blocks = cells // BLK
    face_rows = face_left.shape[0] // BLK
    capacity = send_list.shape[0] // n_sub
    padded = face_rows + 8
    dims = (n_dom, n_sub, capacity, blocks, face_rows)
    f32, i32 = jnp.float32, jnp.int32
    planes = n_dom // (2 if n_dom % 2 == 0 else 1)
    away = -(-((n_sub - 1) * capacity + RIM) // 8) * 8
    sem = pltpu.SemaphoreType.DMA
    operands = (
        send_list,
        by_block(primitive),
        gradient,
        volume.reshape(blocks, BLK),
        face_left.reshape(face_rows, BLK),
        face_right.reshape(face_rows, BLK),
        by_block(face_angles),
        face_area.reshape(face_rows, BLK),
        by_block(face_offsets),
        rim_left.reshape(RIM, BLK),
        rim_right.reshape(RIM, BLK),
        by_block(rim_angles),
        rim_area.reshape(RIM, BLK),
        by_block(rim_offsets),
    )
    vmem = pltpu.VMEM
    rate, new, step = pl.pallas_call(
        functools.partial(kernel, dims),
        out_shape=(
            vmem((blocks, 5, BLK), f32),
            vmem((blocks, 5, BLK), f32),
            pltpu.SMEM((1,), f32),
        ),
        in_specs=[pl.BlockSpec(memory_space=pl.ANY)] * len(operands),
        out_specs=(pl.BlockSpec(memory_space=pltpu.VMEM), pl.BlockSpec(memory_space=pltpu.VMEM), pl.BlockSpec(memory_space=pltpu.SMEM)),
        scratch_shapes=[
            pltpu.SMEM(send_list.shape, i32),
            vmem((blocks, 5, BLK), f32),
            vmem((5, blocks, BLK), f32),
            vmem((blocks, 15, BLK), f32),
            vmem((blocks, BLK), f32),
            vmem((face_rows, BLK), i32),
            vmem((face_rows, BLK), i32),
            vmem((2, padded, BLK), f32),
            vmem((padded, BLK), f32),
            vmem((6, padded, BLK), f32),
            vmem((RIM, BLK), i32),
            vmem((RIM, BLK), i32),
            vmem((n_sub, 20 * capacity, BLK), f32),
            vmem((n_sub, 20 * capacity, BLK), f32),
            vmem((RIM, 5, BLK), f32),
            vmem((RIM, 15, BLK), f32),
            vmem((blocks, 8, BLK), i32),
            vmem((n_sub, capacity, 8, BLK), i32),
            vmem((RIM, 8, BLK), i32),
            vmem((1, BLK), f32),
            vmem((n_dom, n_sub, 1, BLK), f32),
            vmem((n_dom // planes * n_sub, 1, BLK), f32),
            vmem((1, BLK), f32),
            vmem((1, BLK), f32),
            vmem((1, BLK), f32),
            vmem((n_sub, 5, capacity, BLK), f32),
            vmem((n_sub, 5, capacity, BLK), f32),
            vmem((5, RIM, BLK), f32),
            vmem((5, RIM, BLK), f32),
            vmem((padded, BLK), i32),
            vmem((padded, BLK), i32),
            vmem((padded, BLK), i32),
            vmem((padded, BLK), i32),
            vmem((RAW, padded, BLK), f32),
            vmem((PACKED, padded, BLK), i32),
            vmem((RAW, padded, BLK), f32),
            vmem((PACKED, padded, BLK), i32),
            vmem((10, padded, BLK), f32),
            vmem((5 * PIECES, padded, BLK), f32),
            sem((blocks + 30,)),
            sem((n_sub,)),
            sem((n_sub,)),
            sem((2,)),
            sem((2,)),
            sem((planes,)),
            sem((planes,)),
            sem,
            sem,
            sem((n_sub,)),
            sem((n_sub,)),
            sem,
            sem,
            pltpu.SemaphoreType.REGULAR,
            pltpu.SemaphoreType.REGULAR,
        ],
        compiler_params=pltpu.CompilerParams(collective_id=0, has_side_effects=True),
        name="hydro_step",
    )(*operands)
    spaces = (pltpu.VMEM, pltpu.VMEM, pltpu.SMEM)
    rate, new, step = (pltpu.with_memory_space_constraint(x, m) for x, m in zip((rate, new, step), spaces))
    rate, new, step = pl.pallas_call(
        finish,
        out_shape=[jax.ShapeDtypeStruct(x.shape, f32) for x in (rate, new, step)],
        in_specs=[pl.BlockSpec(memory_space=space) for space in spaces],
        out_specs=[pl.BlockSpec(memory_space=pl.ANY)] * 3,
        scratch_shapes=[sem((3,))],
        compiler_params=pltpu.CompilerParams(vmem_limit_bytes=2**20),
        name="finish",
    )(rate, new, step)
    flat = lambda x: x.transpose(1, 0, 2).reshape(5, cells)
    return flat(rate), flat(new), step.reshape(())


def solution(mesh):
    both = ("dom", "sub")
    wide, flat = P(None, both), P(both)
    in_specs = (wide, wide, flat, flat, flat, wide, flat, wide, flat, flat, wide, flat, wide, flat)
    out_specs = (wide, wide, P())
    step = functools.partial(body, (mesh.shape["dom"], mesh.shape["sub"]))
    return jax.shard_map(step, mesh=mesh, in_specs=in_specs, out_specs=out_specs, check_vma=False)
```

```python
import functools
import jax
import jax.numpy as jnp
from jax import lax
from jax.experimental import pallas as pl
from jax.experimental.pallas import tpu as pltpu
from jax.sharding import PartitionSpec as P

BLK = 128
RIM = 4
GROUP = 26
PIECES = 2
WORDS = 10
STEPS = 32767.0
PRIM_STEP = 3.0 / STEPS
GRAD_STEP = 1.5 / STEPS

adiabatic = 5.0 / 3.0
courant = 0.3
MESH = pl.DeviceIdType.MESH


def sin_cos(x):
    turns = jnp.floor(x * 0.63661977236 + 0.5)
    r = (x - turns * 1.57079637050628662109375) - turns * -4.37113900018624283e-8
    r2 = r * r
    sine = r + r * r2 * (-1.6666667163e-1 + r2 * (8.3333337680e-3 + r2 * (-1.9841270114e-4 + r2 * 2.7557314297e-6)))
    cosine = 1.0 + r2 * (-0.5 + r2 * (4.1666667908e-2 + r2 * (-1.3888889225e-3 + r2 * 2.4801587642e-5)))
    odd = jnp.abs(turns) == 1.0
    s = jnp.where(odd, cosine, sine)
    c = jnp.where(odd, sine, cosine)
    s = jnp.where((turns < 0.0) | (turns > 1.0), -s, s)
    c = jnp.where((turns > 0.0) | (turns < -1.0), -c, c)
    return s, c


def pack_pair(a, b, scale_a, scale_b):
    high = (a * scale_a + 32768.5).astype(jnp.int32)
    low = (b * scale_b + 32768.5).astype(jnp.int32)
    return lax.shift_left(high, jnp.full_like(high, 16)) + (low + jnp.int32(-(2**31)))


def pack_block(store, upper, lower, rest):
    mixed = lax.broadcasted_iota(jnp.int32, (8, BLK), 0) == 7
    scale = jnp.where(mixed, 1.0 / PRIM_STEP, 1.0 / GRAD_STEP)
    store(0, 8, pack_pair(upper, lower, 1.0 / GRAD_STEP, scale))
    store(8, 2, pack_pair(rest[0:2], rest[2:4], 1.0 / PRIM_STEP, 1.0 / PRIM_STEP))


def side_state(word, offsets):
    high, low = [], []
    for w in range(WORDS):
        value = word(w)
        high.append(lax.shift_right_arithmetic(value, jnp.full_like(value, 16)).astype(jnp.float32))
        low.append(((value & 65535) - 32768).astype(jnp.float32))
    slope = high[:8] + low[:7]
    centre = [low[7], high[8], high[9], low[8], low[9]]
    offsets = [r * GRAD_STEP for r in offsets]
    values = [centre[c] * PRIM_STEP + dot3(slope[3 * c : 3 * c + 3], offsets) for c in range(5)]
    sound = jnp.exp((values[4] - values[0]) * 0.5) * (adiabatic**0.5)
    return jnp.exp(values[0]), values[1:4], jnp.exp(values[4]), sound


def dot3(a, b):
    return a[0] * b[0] + a[1] * b[1] + a[2] * b[2]


def hllc(normal, left, right):
    dl, vl, pl_, cl, ul = left
    dr, vr, pr, cr = right
    ur = dot3(vr, normal)
    signal_l = jnp.minimum(ul - cl, ur - cr)
    signal_r = jnp.maximum(ul + cl, ur + cr)
    mass_l = dl * (signal_l - ul)
    mass_r = dr * (signal_r - ur)
    contact = (pr - pl_ + mass_l * ul - mass_r * ur) / (mass_l - mass_r)
    outer = signal_l >= 0
    from_left = jnp.logical_or(outer, contact >= 0)
    starred = jnp.where(from_left, signal_l, -signal_r) < 0
    pick = lambda a, b: jnp.where(from_left, a, b)
    density, pressure, speed, sound = pick(dl, dr), pick(pl_, pr), pick(ul, ur), pick(cl, cr)
    velocity = [pick(a, b) for a, b in zip(vl, vr)]
    signal, mass_rate = pick(signal_l, signal_r), pick(mass_l, mass_r)
    specific = sound * sound * (1.0 / (adiabatic * (adiabatic - 1.0))) + 0.5 * dot3(velocity, velocity)
    energy = density * specific
    jump = contact - speed
    factor = mass_rate / (signal - contact)
    rise = jnp.where(starred, signal * (factor - density), 0.0)
    push = jnp.where(starred, signal * factor * jump, 0.0)
    rate = density * speed
    out = [rate + rise]
    along = pressure + push
    carry = rate + rise
    for v, n in zip(velocity, normal):
        out.append(carry * v + along * n)
    out.append((energy + pressure) * speed + rise * specific + push * (contact + pressure / mass_rate))
    return out


def lane_gather(row, index):
    table = jnp.broadcast_to(row, index.shape)
    return jnp.take_along_axis(table, index, axis=1, mode="promise_in_bounds")


def flip(index, mask, size):
    out, bit = index, 1
    while bit < size:
        if mask & bit:
            out = out + bit * (1 - 2 * lax.rem(lax.div(index, bit), 2))
        bit *= 2
    return out


def kernel(
    dims,
    send_hbm,
    prim_rows,
    grad_hbm,
    volume_hbm,
    left_hbm,
    right_hbm,
    angles_hbm,
    area_hbm,
    offsets_hbm,
    rim_left_hbm,
    rim_right_hbm,
    rim_angles_hbm,
    rim_area_hbm,
    rim_offsets_hbm,
    rate_out,
    new_out,
    step_out,
    send_list,
    prim,
    cells,
    grad,
    faces,
    shape,
    load_spare,
    outgoing,
    ghosts,
    next_prim,
    next_grad,
    own_packed,
    ghost_packed,
    next_packed,
    min_own,
    mins,
    min_spare,
    min_base,
    ups,
    gback_send,
    gback_recv,
    rback_send,
    rback_recv,
    hi_left,
    lo_left,
    hi_right,
    lo_right,
    left_words,
    right_words,
    ready,
    pieces,
    load_sem,
    ghost_send_sem,
    ghost_recv_sem,
    rim_send_sem,
    rim_recv_sem,
    min_send_sem,
    min_recv_sem,
    up_send_sem,
    up_recv_sem,
    gback_send_sem,
    gback_recv_sem,
    rback_send_sem,
    rback_recv_sem,
    hello,
    hello_next,
):
    n_dom, n_sub, capacity, blocks, face_rows = dims
    rows = face_rows + RIM
    group = max(k for k in range(1, GROUP + 1) if rows % k == 0)
    ghost_blocks = n_sub * capacity
    me_dom = lax.axis_index("dom")
    me_sub = lax.axis_index("sub")
    plane = 1
    planes = n_dom // plane
    my_plane = lax.div(me_dom, plane)
    base_dom = my_plane * plane
    last = me_dom == n_dom - 1
    first = me_dom == 0
    power = n_sub & (n_sub - 1) == 0

    def to_peer(k):
        return flip(me_sub, k, n_sub) if power else lax.rem(me_sub + k, n_sub)

    def from_peer(k):
        return flip(me_sub, k, n_sub) if power else lax.rem(me_sub + n_sub - k, n_sub)

    far_first = list(range(n_sub - 1, 0, -1))
    near = [1]

    tail = pl.ds(face_rows, RIM)
    body = slice(0, face_rows)
    pairs = [(send_hbm, send_list, 0), (prim_rows, prim, 1)]
    pairs += [(grad_hbm.at[:, h * BLK : (h + 1) * BLK], grad.at[h], 1) for h in range(blocks)]
    pairs += [(prim_rows.at[:, r, :], cells.at[r], 2) for r in range(5)]
    pairs += [(volume_hbm, cells.at[5], 2)]
    middle = len(pairs)
    pairs += [(left_hbm, faces.at[0, body, :], 3), (right_hbm, faces.at[1, body, :], 3)]
    pairs += [(rim_left_hbm, faces.at[0, tail, :], 3), (rim_right_hbm, faces.at[1, tail, :], 3)]
    for where, angle, offset, size in (
        (body, angles_hbm, offsets_hbm, area_hbm),
        (tail, rim_angles_hbm, rim_offsets_hbm, rim_area_hbm),
    ):
        pairs += [(angle.at[:, r, :], shape.at[r, where, :], 4) for r in range(2)]
        pairs += [(offset.at[:, r, :], shape.at[2 + r, where, :], 4) for r in range(6)]
        pairs += [(size, shape.at[8, where, :], 4)]
    loads = [pltpu.make_async_copy(a, b, load_sem.at[k]) for a, b, k in pairs]

    def loaded(k):
        used = slice(0, rows)
        whole = (send_list, load_spare, cells, faces.at[:, used, :], shape.at[:, used, :])[k]
        pltpu.make_async_copy(whole, whole, load_sem.at[k]).wait()

    angles, offsets, area = shape.at[0:2], shape.at[2:8], shape.at[8]
    volume = cells.at[5]
    for load in loads[:middle]:
        load.start()

    barrier = pltpu.get_barrier_semaphore()
    for step in range(plane):
        dom = base_dom + lax.rem(me_dom + step, plane)
        for k in range(n_sub):
            if step or k:
                pl.semaphore_signal(barrier, inc=1, device_id=(dom, to_peer(k)), device_id_type=MESH)

    def greet(p, carry):
        for step in range(plane):
            for k in range(n_sub):
                pl.semaphore_signal(barrier, inc=1, device_id=(p * plane + step, k), device_id_type=MESH)
        return carry

    for load in loads[middle:]:
        load.start()
    lax.fori_loop(my_plane + 1, planes, greet, 0)

    loaded(0)
    loaded(1)
    for k in far_first:
        for j in range(capacity):
            block = jnp.maximum(send_list[to_peer(k) * capacity + j], 0)
            slopes, centres = grad[block], prim[block]
            outgoing[k, 8 * j : 8 * j + 8, :] = slopes[0:8]
            low = 8 * capacity + 8 * j
            outgoing[k, low : low + 7, :] = slopes[8:15]
            outgoing[k, low + 7 : low + 8, :] = centres[0:1]
            outgoing[k, 16 * capacity + 4 * j : 16 * capacity + 4 * j + 4, :] = centres[1:5]

    loaded(2)
    signal = jnp.exp((cells[4] - cells[0]) * 0.5) * (adiabatic**0.5) + jnp.sqrt(
        cells[1] * cells[1] + cells[2] * cells[2] + cells[3] * cells[3]
    )
    limit = jnp.exp(jnp.log(volume[...]) * (1.0 / 3.0)) / signal
    min_own[...] = jnp.min(limit, axis=0, keepdims=True)

    def halves(slopes, centres):
        return slopes[0:8], jnp.concatenate([slopes[8:15], centres[0:1]], 0), centres[1:5]

    for h in range(blocks):

        def store(at, size, value):
            own_packed[h, at : at + size, :] = value

        pack_block(store, *halves(grad[h], prim[h]))

    loaded(3)
    over = pl.ds(face_rows, 8)
    high = lambda x: lax.shift_right_logical(x, jnp.full_like(x, 7))
    for side, hi, lo, shift in ((0, hi_left, lo_left, blocks - RIM), (1, hi_right, lo_right, blocks + ghost_blocks)):
        faces[side, face_rows + RIM : face_rows + 8, :] = faces[side, tail, :]
        hi[body, :] = high(faces[side, body, :])
        lo[...] = faces[side] & (BLK - 1)
        hi[over, :] = high(faces[side, over, :]) + shift

    def row_of(packed):
        return lambda w: packed[w : w + 1, :]

    def gather_into(target, hi, lo, starts, sources, names, keep):
        at = [pl.ds(s, 8) for s in starts]
        index = [lo[here, :] for here in at]
        wanted = [hi[here, :] for here in at]
        match = [[w == name for name in names] for w in wanted]
        for w in range(WORDS):
            values = [target[w, here, :] for here in at] if keep else [None] * len(at)
            for n, row in enumerate(sources):
                line = row(w)
                for i in range(len(at)):
                    got = lane_gather(line, index[i])
                    values[i] = got if values[i] is None else jnp.where(match[i][n], got, values[i])
            for here, value in zip(at, values):
                target[w, here, :] = value

    width = 2 if face_rows % 16 == 0 else 1
    strides = face_rows // (8 * width)

    def gather_main(target, hi, lo, sources, names, keep, begin, end):
        def one(g, carry):
            starts = [pl.multiple_of(g * (8 * width) + 8 * i, 8) for i in range(width)]
            gather_into(target, hi, lo, starts, sources, names, keep)
            return carry

        lax.fori_loop(begin, end, one, 0)

    own = [row_of(own_packed.at[h]) for h in range(blocks)]

    def gather_left(begin, end):
        gather_main(left_words, hi_left, lo_left, own, range(blocks), False, begin, end)

    begun = jnp.where(jnp.logical_and(first, me_sub < 2), max(strides - 1, 0), 0)
    gather_left(0, begun)

    count = plane * n_sub - 1 + plane * n_sub * my_plane
    pl.semaphore_wait(barrier, count)

    def await_all(some, semaphore):
        pltpu.make_async_copy(some, some, semaphore).wait()

    def remote(src, dst, send, recv, dom, sub):
        return pltpu.make_async_remote_copy(
            src_ref=src, dst_ref=dst, send_sem=send, recv_sem=recv, device_id=(dom, sub), device_id_type=MESH
        )

    def min_copy(dom, sub, p):
        here = mins.at[me_dom, me_sub]
        return remote(min_own, here, min_send_sem, min_recv_sem.at[0 if p is None else 1], dom, sub)

    for step in range(plane):
        dom = base_dom + lax.rem(me_dom + step, plane)
        for k in range(n_sub):
            if step or k:
                min_copy(dom, to_peer(k), None).start()

    ghost_copies = {
        k: remote(
            outgoing.at[k], ghosts.at[k], ghost_send_sem, ghost_recv_sem.at[0 if k in near else 1], me_dom, to_peer(k)
        )
        for k in far_first
    }
    for k in far_first:
        ghost_copies[k].start()
    rim_copies = [
        remote(src.at[0:RIM], dst, rim_send_sem, rim_recv_sem, me_dom - 1, me_sub)
        for src, dst in ((prim, next_prim), (grad, next_grad))
    ]

    def tell(p, carry):
        for step in range(plane):
            for k in range(n_sub):
                min_copy(p * plane + step, k, p).start()
        return carry

    @pl.when(jnp.logical_not(first))
    def _():
        for copy in rim_copies:
            copy.start()

    lax.fori_loop(0, my_plane, tell, 0)

    def hail(p, carry):
        there = (lax.rem(me_dom, plane) + p * plane, me_sub)
        pl.semaphore_signal(hello, inc=1, device_id=there, device_id_type=MESH)
        return carry

    lax.fori_loop(0, my_plane, hail, 0)

    @pl.when(jnp.logical_and(lax.rem(me_dom, plane) == 0, me_dom > 0))
    def _():
        pl.semaphore_signal(hello_next, inc=1, device_id=(me_dom - 1, me_sub), device_id_type=MESH)

    gather_left(begun, strides)
    gather_into(left_words, hi_left, lo_left, [face_rows], own[blocks - RIM :], range(blocks - RIM, blocks), False)

    def pack_ghosts(k):
        for j in range(capacity):
            low, rest = 8 * capacity + 8 * j, 16 * capacity + 4 * j

            def store(at, size, value):
                ghost_packed[k, j, at : at + size, :] = value

            pack_block(
                store, ghosts[k, 8 * j : 8 * j + 8, :], ghosts[k, low : low + 8, :], ghosts[k, rest : rest + 4, :]
            )

    def ghost_pass(ks, sources, names):
        await_all(ghosts.at[min(ks) : max(ks) + 1], ghost_recv_sem.at[0 if sources else 1])
        for k in ks:
            pack_ghosts(k)
        more = [row_of(ghost_packed.at[k, j]) for k in ks for j in range(capacity)]
        called = [blocks + from_peer(k) * capacity + j for k in ks for j in range(capacity)]
        gather_main(right_words, hi_right, lo_right, sources + more, names + called, not sources, 0, strides)

    ghost_pass(near, own, list(range(blocks)))

    loaded(4)
    for r in range(9):
        shape[r, face_rows + RIM : face_rows + 8, :] = shape[r, tail, :]

    def left_step(g, carry):
        here = pl.ds(pl.multiple_of(g * 8, 8), 8)
        sin_a, cos_a = sin_cos(angles[0, here, :])
        sin_b, cos_b = sin_cos(angles[1, here, :])
        normal = [sin_a * cos_b, sin_a * sin_b, cos_a]
        density, velocity, pressure, sound = side_state(
            lambda w: left_words[w, here, :],
            [offsets[k, here, :] for k in range(3)],
        )
        values = normal + [density] + velocity + [pressure, sound, dot3(velocity, normal)]
        for k, value in enumerate(values):
            ready[k, here, :] = value
        return carry

    lax.fori_loop(0, (face_rows + 8) // 8, left_step, 0)

    def await_mins(semaphore, count):
        for p in range(planes):
            if count(p) > 0:

                @pl.when(my_plane == p)
                def _():
                    await_all(min_spare.at[0 : count(p)], semaphore)

    def up_copy(p):
        there = lax.rem(me_dom, plane) + p * plane
        return remote(min_base, ups.at[my_plane], up_send_sem, up_recv_sem, there, me_sub)

    def tell_later():
        await_all(min_spare.at[0 : plane * n_sub - 1], min_recv_sem.at[0])
        small = min_own[...]
        for step in range(1, plane * n_sub):
            dom = base_dom + lax.rem(me_dom + step // n_sub, plane)
            sub = lax.rem(me_sub + step, n_sub)
            small = jnp.minimum(small, mins[dom, sub])
        min_base[...] = small

        @pl.when(my_plane < planes - 1)
        def _():
            pl.semaphore_wait(hello, planes - 1 - my_plane)

        def one(p, carry):
            up_copy(p).start()
            return carry

        lax.fori_loop(my_plane + 1, planes, one, 0)

    ghost_pass([k for k in far_first if k not in near], [], [])

    def flux_step(g, carry):
        here = pl.ds(pl.multiple_of(g * 8, 8) if isinstance(g, jax.Array) else g * 8, 8)
        kept = [ready[k, here, :] for k in range(10)]
        right = side_state(
            lambda w: right_words[w, here, :],
            [offsets[k, here, :] for k in range(3, 6)],
        )
        flux = hllc(kept[:3], (kept[3], kept[4:7], kept[7], kept[8], kept[9]), right)
        for c in range(5):
            value = flux[c] * area[here, :]
            if not isinstance(g, jax.Array):
                value = jnp.where(last, 0.0, value)
            big = value.astype(jnp.bfloat16).astype(jnp.float32)
            pieces[c, here, :] = big
            pieces[5 + c, here, :] = value - big
        return carry

    lax.fori_loop(0, face_rows // 8, flux_step, 0)

    @pl.when(last)
    def _():
        next_prim[...] = jnp.zeros_like(next_prim)
        next_grad[...] = jnp.zeros_like(next_grad)

    @pl.when(jnp.logical_not(last))
    def _():
        await_all(load_spare.at[0:RIM], rim_recv_sem)

    for h in range(RIM):
        def store(at, size, value):
            next_packed[h, at : at + size, :] = value

        pack_block(store, *halves(next_grad[h], next_prim[h]))
    start = blocks + ghost_blocks
    gather_into(
        right_words,
        hi_right,
        lo_right,
        [face_rows],
        [row_of(next_packed.at[h]) for h in range(RIM)],
        range(start, start + RIM),
        False,
    )

    flux_step(face_rows // 8, 0)
    tell_later()

    lane_iota = lax.broadcasted_iota(jnp.int32, (BLK, BLK), 0)

    def one_hot(lo, s):
        return jnp.where(lane_iota == lo[pl.ds(s, 1), :], 1.0, 0.0).astype(jnp.bfloat16)

    def spread(hi, s, place, sign):
        match = place == hi[pl.ds(s, 1), :]
        parts = []
        for c in range(5 * PIECES):
            value = pieces[c, pl.ds(s, 1), :]
            value = value if sign > 0 else -value
            parts.append(jnp.where(match, value, 0.0))
        return jnp.concatenate(parts, 0).astype(jnp.bfloat16)

    def product(a, b):
        return lax.dot_general(a, b, (((1,), (1,)), ((), ())), preferred_element_type=jnp.float32)

    def fold(total, count):
        total = total.reshape(PIECES, 5, count, BLK)
        return total[0] + total[1]

    sent = (n_sub - 1) * capacity
    away = -(-(sent + RIM) // 8) * 8
    spot = lax.broadcasted_iota(jnp.int32, (away, BLK), 0)
    away_place = spot - sent + (blocks + ghost_blocks)
    for k in range(1, n_sub):
        lower = (k - 1) * capacity
        away_place = jnp.where(
            (spot >= lower) & (spot < lower + capacity), spot - lower + (blocks + from_peer(k) * capacity), away_place
        )
    own_place = lax.broadcasted_iota(jnp.int32, (blocks, BLK), 0)

    def away_step(i, total):
        a = jnp.concatenate([spread(hi_right, i * group + k, away_place, -1) for k in range(group)], 1)
        b = jnp.concatenate([one_hot(lo_right, i * group + k) for k in range(group)], 1)
        return total + product(a, b)

    total = lax.fori_loop(0, rows // group, away_step, jnp.zeros((5 * PIECES * away, BLK), jnp.float32))
    total = fold(total, away)
    for k in range(1, n_sub):
        gback_send[k] = total[:, (k - 1) * capacity : k * capacity, :]
    rback_send[...] = total[:, sent : sent + RIM, :]
    gback_copies = {
        k: remote(
            gback_send.at[k], gback_recv.at[k], gback_send_sem, gback_recv_sem, me_dom, from_peer(k)
        )
        for k in far_first
    }
    for k in far_first:
        gback_copies[k].start()
    rback_copy = remote(rback_send, rback_recv, rback_send_sem, rback_recv_sem, me_dom + 1, me_sub)

    @pl.when(jnp.logical_and(lax.rem(me_dom, plane) == plane - 1, jnp.logical_not(last)))
    def _():
        pl.semaphore_wait(hello_next, 1)

    @pl.when(jnp.logical_not(last))
    def _():
        rback_copy.start()

    def local_step(i, total):
        a = [spread(hi_left, i * group + k, own_place, 1) for k in range(group)]
        a += [spread(hi_right, i * group + k, own_place, -1) for k in range(group)]
        b = [one_hot(lo_left, i * group + k) for k in range(group)]
        b += [one_hot(lo_right, i * group + k) for k in range(group)]
        return total + product(jnp.concatenate(a, 1), jnp.concatenate(b, 1))

    total = lax.fori_loop(0, rows // group, local_step, jnp.zeros((5 * PIECES * blocks, BLK), jnp.float32))
    net = fold(total, blocks)

    await_mins(up_recv_sem, lambda p: p)
    await_mins(min_recv_sem.at[1], lambda p: plane * n_sub * (planes - 1 - p))

    def earlier(p, small):
        return jnp.minimum(small, ups[p])

    smallest = lax.fori_loop(0, my_plane, earlier, min_base[...])

    def later(p, small):
        for step in range(plane):
            for k in range(n_sub):
                small = jnp.minimum(small, mins[p * plane + step, k])
        return small

    smallest = lax.fori_loop(my_plane + 1, planes, later, smallest)
    time_step = courant * jnp.min(smallest, axis=1, keepdims=True)
    step_out[0] = courant * jnp.min(smallest)

    @pl.when(first)
    def _():
        rback_recv[...] = jnp.zeros_like(rback_recv)

    @pl.when(jnp.logical_not(first))
    def _():
        rback_copy.wait_recv()

    await_all(gback_recv.at[1:n_sub], gback_recv_sem)

    square = cells[1] * cells[1] + cells[2] * cells[2] + cells[3] * cells[3]
    density = jnp.exp(cells[0])
    energy = jnp.exp(cells[4]) / (adiabatic - 1.0) + 0.5 * density * square
    conserved = [density, density * cells[1], density * cells[2], density * cells[3], energy]
    inverse = -1.0 / volume[...]
    for c in range(5):
        sums = net[c]
        for h in range(RIM):
            sums = sums + jnp.where(own_place == h, rback_recv[c, h : h + 1, :], 0.0)
        for k in range(1, n_sub):
            for j in range(capacity):
                wanted = send_list[to_peer(k) * capacity + j]
                sums = sums + jnp.where(own_place == wanted, gback_recv[k, c, j : j + 1, :], 0.0)
        rate = sums * inverse
        new = conserved[c] + time_step * rate
        rate_out[:, c, :] = rate
        new_out[:, c, :] = new

    @pl.when(jnp.logical_not(first))
    def _():
        await_all(load_spare.at[0:RIM], rim_send_sem)

    @pl.when(jnp.logical_not(last))
    def _():
        rback_copy.wait_send()

    await_all(ghosts.at[1:n_sub], ghost_send_sem)
    await_all(gback_recv.at[1:n_sub], gback_send_sem)
    await_mins(min_send_sem, lambda p: plane * n_sub * (p + 1) - 1)
    await_mins(up_send_sem, lambda p: planes - 1 - p)


def finish(rate, new, step, rate_out, new_out, step_out, sems):
    pairs = ((rate, rate_out), (new, new_out), (step, step_out))
    copies = [pltpu.make_async_copy(a, b, sems.at[k]) for k, (a, b) in enumerate(pairs)]
    for copy in copies:
        copy.start()
    for copy in copies:
        copy.wait()


def by_block(x):
    return x.reshape(x.shape[0], x.shape[1] // BLK, BLK).transpose(1, 0, 2)


def body(mesh_sizes, *args):
    (primitive, gradient, volume, face_left, face_right, face_angles, face_area, face_offsets) = args[:8]
    (rim_left, rim_right, rim_angles, rim_area, rim_offsets, send_list) = args[8:]
    n_dom, n_sub = mesh_sizes
    cells = primitive.shape[1]
    blocks = cells // BLK
    face_rows = face_left.shape[0] // BLK
    capacity = send_list.shape[0] // n_sub
    padded = face_rows + 8
    dims = (n_dom, n_sub, capacity, blocks, face_rows)
    f32, i32 = jnp.float32, jnp.int32
    planes = n_dom
    away = -(-((n_sub - 1) * capacity + RIM) // 8) * 8
    sem = pltpu.SemaphoreType.DMA
    operands = (
        send_list,
        by_block(primitive),
        gradient,
        volume.reshape(blocks, BLK),
        face_left.reshape(face_rows, BLK),
        face_right.reshape(face_rows, BLK),
        by_block(face_angles),
        face_area.reshape(face_rows, BLK),
        by_block(face_offsets),
        rim_left.reshape(RIM, BLK),
        rim_right.reshape(RIM, BLK),
        by_block(rim_angles),
        rim_area.reshape(RIM, BLK),
        by_block(rim_offsets),
    )
    vmem = pltpu.VMEM
    rate, new, step = pl.pallas_call(
        functools.partial(kernel, dims),
        out_shape=(
            vmem((blocks, 5, BLK), f32),
            vmem((blocks, 5, BLK), f32),
            pltpu.SMEM((1,), f32),
        ),
        in_specs=[pl.BlockSpec(memory_space=pl.ANY)] * len(operands),
        out_specs=(pl.BlockSpec(memory_space=pltpu.VMEM), pl.BlockSpec(memory_space=pltpu.VMEM), pl.BlockSpec(memory_space=pltpu.SMEM)),
        scratch_shapes=[
            pltpu.SMEM(send_list.shape, i32),
            vmem((blocks, 5, BLK), f32),
            vmem((6, blocks, BLK), f32),
            vmem((blocks, 15, BLK), f32),
            vmem((2, padded, BLK), i32),
            vmem((9, padded, BLK), f32),
            vmem((blocks, 20, BLK), f32),
            vmem((n_sub, 20 * capacity, BLK), f32),
            vmem((n_sub, 20 * capacity, BLK), f32),
            vmem((RIM, 5, BLK), f32),
            vmem((RIM, 15, BLK), f32),
            vmem((blocks, 16, BLK), i32),
            vmem((n_sub, capacity, 16, BLK), i32),
            vmem((RIM, 16, BLK), i32),
            vmem((1, BLK), f32),
            vmem((n_dom, n_sub, 1, BLK), f32),
            vmem((n_dom * n_sub, 1, BLK), f32),
            vmem((1, BLK), f32),
            vmem((planes, 1, BLK), f32),
            vmem((n_sub, 5, capacity, BLK), f32),
            vmem((n_sub, 5, capacity, BLK), f32),
            vmem((5, RIM, BLK), f32),
            vmem((5, RIM, BLK), f32),
            vmem((padded, BLK), i32),
            vmem((padded, BLK), i32),
            vmem((padded, BLK), i32),
            vmem((padded, BLK), i32),
            vmem((WORDS, padded, BLK), i32),
            vmem((WORDS, padded, BLK), i32),
            vmem((10, padded, BLK), f32),
            vmem((5 * PIECES, padded, BLK), f32),
            sem((5,)),
            sem,
            sem((2,)),
            sem,
            sem,
            sem,
            sem((2,)),
            sem,
            sem,
            sem,
            sem,
            sem,
            sem,
            pltpu.SemaphoreType.REGULAR,
            pltpu.SemaphoreType.REGULAR,
        ],
        compiler_params=pltpu.CompilerParams(collective_id=0, has_side_effects=True),
        name="hydro_step",
    )(*operands)
    spaces = (pltpu.VMEM, pltpu.VMEM, pltpu.SMEM)
    rate, new, step = (pltpu.with_memory_space_constraint(x, m) for x, m in zip((rate, new, step), spaces))
    rate, new, step = pl.pallas_call(
        finish,
        out_shape=[jax.ShapeDtypeStruct(x.shape, f32) for x in (rate, new, step)],
        in_specs=[pl.BlockSpec(memory_space=space) for space in spaces],
        out_specs=[pl.BlockSpec(memory_space=pl.ANY)] * 3,
        scratch_shapes=[sem((3,))],
        compiler_params=pltpu.CompilerParams(vmem_limit_bytes=2**20),
        name="finish",
    )(rate, new, step)
    flat = lambda x: x.transpose(1, 0, 2).reshape(5, cells)
    return flat(rate), flat(new), step.reshape(())


def solution(mesh):
    both = ("dom", "sub")
    wide, flat = P(None, both), P(both)
    in_specs = (wide, wide, flat, flat, flat, wide, flat, wide, flat, flat, wide, flat, wide, flat)
    out_specs = (wide, wide, P())
    step = functools.partial(body, (mesh.shape["dom"], mesh.shape["sub"]))
    return jax.shard_map(step, mesh=mesh, in_specs=in_specs, out_specs=out_specs, check_vma=False)
```

```python
import functools
import jax
import jax.numpy as jnp
from jax import lax
from jax.experimental import pallas as pl
from jax.experimental.pallas import tpu as pltpu
from jax.sharding import PartitionSpec as P

BLK = 128
RIM = 4
GROUP = 26
PIECES = 2
WORDS = 10
STEPS = 32767.0
PRIM_STEP = 3.0 / STEPS
GRAD_STEP = 1.5 / STEPS

adiabatic = 5.0 / 3.0
courant = 0.3
MESH = pl.DeviceIdType.MESH


def sin_cos(x):
    turns = jnp.floor(x * 0.63661977236 + 0.5)
    r = (x - turns * 1.57079637050628662109375) - turns * -4.37113900018624283e-8
    r2 = r * r
    sine = r + r * r2 * (-1.6666667163e-1 + r2 * (8.3333337680e-3 + r2 * (-1.9841270114e-4 + r2 * 2.7557314297e-6)))
    cosine = 1.0 + r2 * (-0.5 + r2 * (4.1666667908e-2 + r2 * (-1.3888889225e-3 + r2 * 2.4801587642e-5)))
    odd = jnp.abs(turns) == 1.0
    s = jnp.where(odd, cosine, sine)
    c = jnp.where(odd, sine, cosine)
    s = jnp.where((turns < 0.0) | (turns > 1.0), -s, s)
    c = jnp.where((turns > 0.0) | (turns < -1.0), -c, c)
    return s, c


def pack_pair(a, b, scale_a, scale_b):
    high = (a * scale_a + 32768.5).astype(jnp.int32)
    low = (b * scale_b + 32768.5).astype(jnp.int32)
    return lax.shift_left(high, jnp.full_like(high, 16)) + (low + jnp.int32(-(2**31)))


def pack_block(store, upper, lower, rest):
    mixed = lax.broadcasted_iota(jnp.int32, (8, BLK), 0) == 7
    scale = jnp.where(mixed, 1.0 / PRIM_STEP, 1.0 / GRAD_STEP)
    store(0, 8, pack_pair(upper, lower, 1.0 / GRAD_STEP, scale))
    store(8, 2, pack_pair(rest[0:2], rest[2:4], 1.0 / PRIM_STEP, 1.0 / PRIM_STEP))


def side_state(word, offsets):
    high, low = [], []
    for w in range(WORDS):
        value = word(w)
        high.append(lax.shift_right_arithmetic(value, jnp.full_like(value, 16)).astype(jnp.float32))
        low.append(((value & 65535) - 32768).astype(jnp.float32))
    slope = high[:8] + low[:7]
    centre = [low[7], high[8], high[9], low[8], low[9]]
    offsets = [r * GRAD_STEP for r in offsets]
    values = [centre[c] * PRIM_STEP + dot3(slope[3 * c : 3 * c + 3], offsets) for c in range(5)]
    sound = jnp.exp((values[4] - values[0]) * 0.5) * (adiabatic**0.5)
    return jnp.exp(values[0]), values[1:4], jnp.exp(values[4]), sound


def dot3(a, b):
    return a[0] * b[0] + a[1] * b[1] + a[2] * b[2]


def hllc(normal, left, right):
    dl, vl, pl_, cl, ul = left
    dr, vr, pr, cr = right
    ur = dot3(vr, normal)
    signal_l = jnp.minimum(ul - cl, ur - cr)
    signal_r = jnp.maximum(ul + cl, ur + cr)
    mass_l = dl * (signal_l - ul)
    mass_r = dr * (signal_r - ur)
    contact = (pr - pl_ + mass_l * ul - mass_r * ur) / (mass_l - mass_r)
    outer = signal_l >= 0
    from_left = jnp.logical_or(outer, contact >= 0)
    starred = jnp.where(from_left, signal_l, -signal_r) < 0
    pick = lambda a, b: jnp.where(from_left, a, b)
    density, pressure, speed, sound = pick(dl, dr), pick(pl_, pr), pick(ul, ur), pick(cl, cr)
    velocity = [pick(a, b) for a, b in zip(vl, vr)]
    signal, mass_rate = pick(signal_l, signal_r), pick(mass_l, mass_r)
    specific = sound * sound * (1.0 / (adiabatic * (adiabatic - 1.0))) + 0.5 * dot3(velocity, velocity)
    energy = density * specific
    jump = contact - speed
    factor = mass_rate / (signal - contact)
    rise = jnp.where(starred, signal * (factor - density), 0.0)
    push = jnp.where(starred, signal * factor * jump, 0.0)
    rate = density * speed
    out = [rate + rise]
    along = pressure + push
    carry = rate + rise
    for v, n in zip(velocity, normal):
        out.append(carry * v + along * n)
    out.append((energy + pressure) * speed + rise * specific + push * (contact + pressure / mass_rate))
    return out


def lane_gather(row, index):
    table = jnp.broadcast_to(row, index.shape)
    return jnp.take_along_axis(table, index, axis=1, mode="promise_in_bounds")


def flip(index, mask, size):
    out, bit = index, 1
    while bit < size:
        if mask & bit:
            out = out + bit * (1 - 2 * lax.rem(lax.div(index, bit), 2))
        bit *= 2
    return out


def kernel(
    dims,
    send_hbm,
    prim_rows,
    grad_hbm,
    volume_hbm,
    left_hbm,
    right_hbm,
    angles_hbm,
    area_hbm,
    offsets_hbm,
    rim_left_hbm,
    rim_right_hbm,
    rim_angles_hbm,
    rim_area_hbm,
    rim_offsets_hbm,
    rate_out,
    new_out,
    step_out,
    send_list,
    prim,
    cells,
    grad,
    faces,
    shape,
    load_spare,
    outgoing,
    ghosts,
    next_prim,
    next_grad,
    own_packed,
    ghost_packed,
    next_packed,
    min_own,
    mins,
    min_spare,
    min_base,
    ups,
    gback_send,
    gback_recv,
    rback_send,
    rback_recv,
    hi_left,
    lo_left,
    hi_right,
    lo_right,
    left_words,
    right_words,
    ready,
    pieces,
    load_sem,
    ghost_send_sem,
    ghost_recv_sem,
    rim_send_sem,
    rim_recv_sem,
    min_send_sem,
    min_recv_sem,
    up_send_sem,
    up_recv_sem,
    gback_send_sem,
    gback_recv_sem,
    rback_send_sem,
    rback_recv_sem,
    hello,
    hello_next,
):
    n_dom, n_sub, capacity, blocks, face_rows = dims
    rows = face_rows + RIM
    group = max(k for k in range(1, GROUP + 1) if rows % k == 0)
    ghost_blocks = n_sub * capacity
    me_dom = lax.axis_index("dom")
    me_sub = lax.axis_index("sub")
    plane = 1
    planes = n_dom // plane
    my_plane = lax.div(me_dom, plane)
    base_dom = my_plane * plane
    last = me_dom == n_dom - 1
    first = me_dom == 0
    power = n_sub & (n_sub - 1) == 0

    def to_peer(k):
        return flip(me_sub, k, n_sub) if power else lax.rem(me_sub + k, n_sub)

    def from_peer(k):
        return flip(me_sub, k, n_sub) if power else lax.rem(me_sub + n_sub - k, n_sub)

    far_first = list(range(n_sub - 1, 0, -1))
    near = [1]

    tail = pl.ds(face_rows, RIM)
    body = slice(0, face_rows)
    pairs = [(send_hbm, send_list, 0), (prim_rows, prim, 1)]
    pairs += [(grad_hbm.at[:, h * BLK : (h + 1) * BLK], grad.at[h], 1) for h in range(blocks)]
    pairs += [(prim_rows.at[:, r, :], cells.at[r], 2) for r in range(5)]
    pairs += [(volume_hbm, cells.at[5], 2)]
    middle = len(pairs)
    pairs += [(left_hbm, faces.at[0, body, :], 3), (right_hbm, faces.at[1, body, :], 3)]
    pairs += [(rim_left_hbm, faces.at[0, tail, :], 3), (rim_right_hbm, faces.at[1, tail, :], 3)]
    for where, angle, offset, size in (
        (body, angles_hbm, offsets_hbm, area_hbm),
        (tail, rim_angles_hbm, rim_offsets_hbm, rim_area_hbm),
    ):
        pairs += [(angle.at[:, r, :], shape.at[r, where, :], 4) for r in range(2)]
        pairs += [(offset.at[:, r, :], shape.at[2 + r, where, :], 4) for r in range(6)]
        pairs += [(size, shape.at[8, where, :], 4)]
    loads = [pltpu.make_async_copy(a, b, load_sem.at[k]) for a, b, k in pairs]

    def loaded(k):
        used = slice(0, rows)
        whole = (send_list, load_spare, cells, faces.at[:, used, :], shape.at[:, used, :])[k]
        pltpu.make_async_copy(whole, whole, load_sem.at[k]).wait()

    angles, offsets, area = shape.at[0:2], shape.at[2:8], shape.at[8]
    volume = cells.at[5]
    for load in loads[:middle]:
        load.start()

    barrier = pltpu.get_barrier_semaphore()
    for step in range(plane):
        dom = base_dom + lax.rem(me_dom + step, plane)
        for k in range(n_sub):
            if step or k:
                pl.semaphore_signal(barrier, inc=1, device_id=(dom, to_peer(k)), device_id_type=MESH)

    def greet(p, carry):
        for step in range(plane):
            for k in range(n_sub):
                pl.semaphore_signal(barrier, inc=1, device_id=(p * plane + step, k), device_id_type=MESH)
        return carry

    for load in loads[middle:]:
        load.start()
    lax.fori_loop(my_plane + 1, planes, greet, 0)

    loaded(0)
    loaded(1)
    for k in far_first:
        for j in range(capacity):
            block = jnp.maximum(send_list[to_peer(k) * capacity + j], 0)
            slopes, centres = grad[block], prim[block]
            outgoing[k, 8 * j : 8 * j + 8, :] = slopes[0:8]
            low = 8 * capacity + 8 * j
            outgoing[k, low : low + 7, :] = slopes[8:15]
            outgoing[k, low + 7 : low + 8, :] = centres[0:1]
            outgoing[k, 16 * capacity + 4 * j : 16 * capacity + 4 * j + 4, :] = centres[1:5]

    loaded(2)
    signal = jnp.exp((cells[4] - cells[0]) * 0.5) * (adiabatic**0.5) + jnp.sqrt(
        cells[1] * cells[1] + cells[2] * cells[2] + cells[3] * cells[3]
    )
    limit = jnp.exp(jnp.log(volume[...]) * (1.0 / 3.0)) / signal
    min_own[...] = jnp.min(limit, axis=0, keepdims=True)

    def halves(slopes, centres):
        return slopes[0:8], jnp.concatenate([slopes[8:15], centres[0:1]], 0), centres[1:5]

    for h in range(blocks):

        def store(at, size, value):
            own_packed[h, at : at + size, :] = value

        pack_block(store, *halves(grad[h], prim[h]))

    loaded(3)
    over = pl.ds(face_rows, 8)
    high = lambda x: lax.shift_right_logical(x, jnp.full_like(x, 7))
    for side, hi, lo, shift in ((0, hi_left, lo_left, blocks - RIM), (1, hi_right, lo_right, blocks + ghost_blocks)):
        faces[side, face_rows + RIM : face_rows + 8, :] = faces[side, tail, :]
        hi[body, :] = high(faces[side, body, :])
        lo[...] = faces[side] & (BLK - 1)
        hi[over, :] = high(faces[side, over, :]) + shift

    def row_of(packed):
        return lambda w: packed[w : w + 1, :]

    def gather_into(target, hi, lo, starts, sources, names, keep):
        at = [pl.ds(s, 8) for s in starts]
        index = [lo[here, :] for here in at]
        wanted = [hi[here, :] for here in at]
        match = [[w == name for name in names] for w in wanted]
        for w in range(WORDS):
            values = [target[w, here, :] for here in at] if keep else [None] * len(at)
            for n, row in enumerate(sources):
                line = row(w)
                for i in range(len(at)):
                    got = lane_gather(line, index[i])
                    values[i] = got if values[i] is None else jnp.where(match[i][n], got, values[i])
            for here, value in zip(at, values):
                target[w, here, :] = value

    width = 2 if face_rows % 16 == 0 else 1
    strides = face_rows // (8 * width)

    def gather_main(target, hi, lo, sources, names, keep, begin, end):
        def one(g, carry):
            starts = [pl.multiple_of(g * (8 * width) + 8 * i, 8) for i in range(width)]
            gather_into(target, hi, lo, starts, sources, names, keep)
            return carry

        lax.fori_loop(begin, end, one, 0)

    own = [row_of(own_packed.at[h]) for h in range(blocks)]

    def gather_left(begin, end):
        gather_main(left_words, hi_left, lo_left, own, range(blocks), False, begin, end)

    begun = jnp.where(jnp.logical_and(first, me_sub < 2), max(strides - 1, 0), 0)
    gather_left(0, begun)

    count = plane * n_sub - 1 + plane * n_sub * my_plane
    pl.semaphore_wait(barrier, count)

    def await_all(some, semaphore):
        pltpu.make_async_copy(some, some, semaphore).wait()

    def remote(src, dst, send, recv, dom, sub):
        return pltpu.make_async_remote_copy(
            src_ref=src, dst_ref=dst, send_sem=send, recv_sem=recv, device_id=(dom, sub), device_id_type=MESH
        )

    def min_copy(dom, sub, p):
        here = mins.at[me_dom, me_sub]
        return remote(min_own, here, min_send_sem, min_recv_sem.at[0 if p is None else 1], dom, sub)

    for step in range(plane):
        dom = base_dom + lax.rem(me_dom + step, plane)
        for k in range(n_sub):
            if step or k:
                min_copy(dom, to_peer(k), None).start()

    ghost_copies = {
        k: remote(
            outgoing.at[k], ghosts.at[k], ghost_send_sem, ghost_recv_sem.at[0 if k in near else 1], me_dom, to_peer(k)
        )
        for k in far_first
    }
    for k in far_first:
        ghost_copies[k].start()
    rim_copies = [
        remote(src.at[0:RIM], dst, rim_send_sem, rim_recv_sem, me_dom - 1, me_sub)
        for src, dst in ((prim, next_prim), (grad, next_grad))
    ]

    def tell(p, carry):
        for step in range(plane):
            for k in range(n_sub):
                min_copy(p * plane + step, k, p).start()
        return carry

    @pl.when(jnp.logical_not(first))
    def _():
        for copy in rim_copies:
            copy.start()

    lax.fori_loop(0, my_plane, tell, 0)

    def hail(p, carry):
        there = (lax.rem(me_dom, plane) + p * plane, me_sub)
        pl.semaphore_signal(hello, inc=1, device_id=there, device_id_type=MESH)
        return carry

    lax.fori_loop(0, my_plane, hail, 0)

    @pl.when(jnp.logical_and(lax.rem(me_dom, plane) == 0, me_dom > 0))
    def _():
        pl.semaphore_signal(hello_next, inc=1, device_id=(me_dom - 1, me_sub), device_id_type=MESH)

    gather_left(begun, strides)
    gather_into(left_words, hi_left, lo_left, [face_rows], own[blocks - RIM :], range(blocks - RIM, blocks), False)

    def pack_ghosts(k):
        for j in range(capacity):
            low, rest = 8 * capacity + 8 * j, 16 * capacity + 4 * j

            def store(at, size, value):
                ghost_packed[k, j, at : at + size, :] = value

            pack_block(
                store, ghosts[k, 8 * j : 8 * j + 8, :], ghosts[k, low : low + 8, :], ghosts[k, rest : rest + 4, :]
            )

    def arrived(ks, semaphore):
        await_all(ghosts.at[min(ks) : max(ks) + 1], semaphore)
        for k in ks:
            pack_ghosts(k)
        lines = [row_of(ghost_packed.at[k, j]) for k in ks for j in range(capacity)]
        return lines, [blocks + from_peer(k) * capacity + j for k in ks for j in range(capacity)]

    more, called = arrived(near, ghost_recv_sem.at[0])
    sources, names = own + more, list(range(blocks)) + called
    gather_main(right_words, hi_right, lo_right, sources, names, False, 0, strides)

    loaded(4)
    for r in range(9):
        shape[r, face_rows + RIM : face_rows + 8, :] = shape[r, tail, :]

    def left_step(g, carry):
        here = pl.ds(pl.multiple_of(g * 8, 8), 8)
        sin_a, cos_a = sin_cos(angles[0, here, :])
        sin_b, cos_b = sin_cos(angles[1, here, :])
        normal = [sin_a * cos_b, sin_a * sin_b, cos_a]
        density, velocity, pressure, sound = side_state(
            lambda w: left_words[w, here, :],
            [offsets[k, here, :] for k in range(3)],
        )
        values = normal + [density] + velocity + [pressure, sound, dot3(velocity, normal)]
        for k, value in enumerate(values):
            ready[k, here, :] = value
        return carry

    lax.fori_loop(0, (face_rows + 8) // 8, left_step, 0)


    @pl.when(last)
    def _():
        next_prim[...] = jnp.zeros_like(next_prim)
        next_grad[...] = jnp.zeros_like(next_grad)

    @pl.when(jnp.logical_not(last))
    def _():
        await_all(load_spare.at[0:RIM], rim_recv_sem)

    for h in range(RIM):
        def store(at, size, value):
            next_packed[h, at : at + size, :] = value

        pack_block(store, *halves(next_grad[h], next_prim[h]))
    def flux_step(g):
        here = pl.ds(g * 8, 8)
        kept = [ready[k, here, :] for k in range(10)]
        right = side_state(
            lambda w: right_words[w, here, :],
            [offsets[k, here, :] for k in range(3, 6)],
        )
        flux = hllc(kept[:3], (kept[3], kept[4:7], kept[7], kept[8], kept[9]), right)
        for c in range(5):
            value = flux[c] * area[here, :]
            if g * 8 >= face_rows:
                value = jnp.where(last, 0.0, value)
            big = value.astype(jnp.bfloat16).astype(jnp.float32)
            pieces[c, here, :] = big
            pieces[5 + c, here, :] = value - big

    lane_iota = lax.broadcasted_iota(jnp.int32, (BLK, BLK), 0)

    def one_hot(lo, s):
        return jnp.where(lane_iota == lo[pl.ds(s, 1), :], 1.0, 0.0).astype(jnp.bfloat16)

    def spread(hi, s, place, sign):
        match = place == hi[pl.ds(s, 1), :]
        parts = []
        for c in range(5 * PIECES):
            value = pieces[c, pl.ds(s, 1), :]
            value = value if sign > 0 else -value
            parts.append(jnp.where(match, value, 0.0))
        return jnp.concatenate(parts, 0).astype(jnp.bfloat16)

    def product(a, b):
        return lax.dot_general(a, b, (((1,), (1,)), ((), ())), preferred_element_type=jnp.float32)

    def fold(total, count):
        total = total.reshape(PIECES, 5, count, BLK)
        return total[0] + total[1]

    sent = (n_sub - 1) * capacity
    away = -(-(sent + RIM) // 8) * 8
    spot = lax.broadcasted_iota(jnp.int32, (away, BLK), 0)
    away_place = spot - sent + (blocks + ghost_blocks)
    for k in range(1, n_sub):
        lower = (k - 1) * capacity
        away_place = jnp.where(
            (spot >= lower) & (spot < lower + capacity), spot - lower + (blocks + from_peer(k) * capacity), away_place
        )
    own_place = lax.broadcasted_iota(jnp.int32, (blocks, BLK), 0)

    def away_rows(which):
        a = jnp.concatenate([spread(hi_right, s, away_place, -1) for s in which], 1)
        b = jnp.concatenate([one_hot(lo_right, s) for s in which], 1)
        return product(a, b)

    def rim_rows():
        start = blocks + ghost_blocks
        gather_into(
            right_words,
            hi_right,
            lo_right,
            [face_rows],
            [row_of(next_packed.at[h]) for h in range(RIM)],
            range(start, start + RIM),
            False,
        )


    lines, called = arrived([k for k in far_first if k not in near], ghost_recv_sem.at[1])
    total = jnp.zeros((5 * PIECES * away, BLK), jnp.float32)
    span = 8 * width
    for t in range(strides + 2):
        if t < strides:
            at = [t * span + 8 * i for i in range(width)]
            gather_into(right_words, hi_right, lo_right, at, lines, called, True)
        if t == strides - 1:
            rim_rows()
        if 1 <= t <= strides:
            for i in range(width):
                flux_step((t - 1) * width + i)
        if t == strides:
            flux_step(face_rows // 8)
        if t >= 2:
            total = total + away_rows(range((t - 2) * span, (t - 1) * span + (RIM if t == strides + 1 else 0)))
    total = fold(total, away)
    for k in range(1, n_sub):
        gback_send[k] = total[:, (k - 1) * capacity : k * capacity, :]
    rback_send[...] = total[:, sent : sent + RIM, :]
    gback_copies = {
        k: remote(
            gback_send.at[k], gback_recv.at[k], gback_send_sem, gback_recv_sem, me_dom, from_peer(k)
        )
        for k in far_first
    }
    for k in far_first:
        gback_copies[k].start()
    rback_copy = remote(rback_send, rback_recv, rback_send_sem, rback_recv_sem, me_dom + 1, me_sub)

    @pl.when(jnp.logical_and(lax.rem(me_dom, plane) == plane - 1, jnp.logical_not(last)))
    def _():
        pl.semaphore_wait(hello_next, 1)

    @pl.when(jnp.logical_not(last))
    def _():
        rback_copy.start()

    def await_mins(semaphore, count):
        for p in range(planes):
            if count(p) > 0:

                @pl.when(my_plane == p)
                def _():
                    await_all(min_spare.at[0 : count(p)], semaphore)

    def up_copy(p):
        there = lax.rem(me_dom, plane) + p * plane
        return remote(min_base, ups.at[my_plane], up_send_sem, up_recv_sem, there, me_sub)

    def tell_later():
        await_all(min_spare.at[0 : plane * n_sub - 1], min_recv_sem.at[0])
        small = min_own[...]
        for step in range(1, plane * n_sub):
            dom = base_dom + lax.rem(me_dom + step // n_sub, plane)
            sub = lax.rem(me_sub + step, n_sub)
            small = jnp.minimum(small, mins[dom, sub])
        min_base[...] = small

        @pl.when(my_plane < planes - 1)
        def _():
            pl.semaphore_wait(hello, planes - 1 - my_plane)

        def one(p, carry):
            up_copy(p).start()
            return carry

        lax.fori_loop(my_plane + 1, planes, one, 0)

    tell_later()

    def local_step(i, total):
        a = [spread(hi_left, i * group + k, own_place, 1) for k in range(group)]
        a += [spread(hi_right, i * group + k, own_place, -1) for k in range(group)]
        b = [one_hot(lo_left, i * group + k) for k in range(group)]
        b += [one_hot(lo_right, i * group + k) for k in range(group)]
        return total + product(jnp.concatenate(a, 1), jnp.concatenate(b, 1))

    total = lax.fori_loop(0, rows // group, local_step, jnp.zeros((5 * PIECES * blocks, BLK), jnp.float32))
    net = fold(total, blocks)

    await_mins(up_recv_sem, lambda p: p)
    await_mins(min_recv_sem.at[1], lambda p: plane * n_sub * (planes - 1 - p))

    def earlier(p, small):
        return jnp.minimum(small, ups[p])

    smallest = lax.fori_loop(0, my_plane, earlier, min_base[...])

    def later(p, small):
        for step in range(plane):
            for k in range(n_sub):
                small = jnp.minimum(small, mins[p * plane + step, k])
        return small

    smallest = lax.fori_loop(my_plane + 1, planes, later, smallest)
    time_step = courant * jnp.min(smallest, axis=1, keepdims=True)
    step_out[0] = courant * jnp.min(smallest)

    @pl.when(first)
    def _():
        rback_recv[...] = jnp.zeros_like(rback_recv)

    @pl.when(jnp.logical_not(first))
    def _():
        rback_copy.wait_recv()

    await_all(gback_recv.at[1:n_sub], gback_recv_sem)

    square = cells[1] * cells[1] + cells[2] * cells[2] + cells[3] * cells[3]
    density = jnp.exp(cells[0])
    energy = jnp.exp(cells[4]) / (adiabatic - 1.0) + 0.5 * density * square
    conserved = [density, density * cells[1], density * cells[2], density * cells[3], energy]
    inverse = -1.0 / volume[...]
    for c in range(5):
        sums = net[c]
        for h in range(RIM):
            sums = sums + jnp.where(own_place == h, rback_recv[c, h : h + 1, :], 0.0)
        for k in range(1, n_sub):
            for j in range(capacity):
                wanted = send_list[to_peer(k) * capacity + j]
                sums = sums + jnp.where(own_place == wanted, gback_recv[k, c, j : j + 1, :], 0.0)
        rate = sums * inverse
        new = conserved[c] + time_step * rate
        rate_out[:, c, :] = rate
        new_out[:, c, :] = new

    @pl.when(jnp.logical_not(first))
    def _():
        await_all(load_spare.at[0:RIM], rim_send_sem)

    @pl.when(jnp.logical_not(last))
    def _():
        rback_copy.wait_send()

    await_all(ghosts.at[1:n_sub], ghost_send_sem)
    await_all(gback_recv.at[1:n_sub], gback_send_sem)
    await_mins(min_send_sem, lambda p: plane * n_sub * (p + 1) - 1)
    await_mins(up_send_sem, lambda p: planes - 1 - p)


def finish(rate, new, step, rate_out, new_out, step_out, sems):
    pairs = ((rate, rate_out), (new, new_out), (step, step_out))
    copies = [pltpu.make_async_copy(a, b, sems.at[k]) for k, (a, b) in enumerate(pairs)]
    for copy in copies:
        copy.start()
    for copy in copies:
        copy.wait()


def by_block(x):
    return x.reshape(x.shape[0], x.shape[1] // BLK, BLK).transpose(1, 0, 2)


def body(mesh_sizes, *args):
    (primitive, gradient, volume, face_left, face_right, face_angles, face_area, face_offsets) = args[:8]
    (rim_left, rim_right, rim_angles, rim_area, rim_offsets, send_list) = args[8:]
    n_dom, n_sub = mesh_sizes
    cells = primitive.shape[1]
    blocks = cells // BLK
    face_rows = face_left.shape[0] // BLK
    capacity = send_list.shape[0] // n_sub
    padded = face_rows + 8
    dims = (n_dom, n_sub, capacity, blocks, face_rows)
    f32, i32 = jnp.float32, jnp.int32
    planes = n_dom
    away = -(-((n_sub - 1) * capacity + RIM) // 8) * 8
    sem = pltpu.SemaphoreType.DMA
    operands = (
        send_list,
        by_block(primitive),
        gradient,
        volume.reshape(blocks, BLK),
        face_left.reshape(face_rows, BLK),
        face_right.reshape(face_rows, BLK),
        by_block(face_angles),
        face_area.reshape(face_rows, BLK),
        by_block(face_offsets),
        rim_left.reshape(RIM, BLK),
        rim_right.reshape(RIM, BLK),
        by_block(rim_angles),
        rim_area.reshape(RIM, BLK),
        by_block(rim_offsets),
    )
    vmem = pltpu.VMEM
    rate, new, step = pl.pallas_call(
        functools.partial(kernel, dims),
        out_shape=(
            vmem((blocks, 5, BLK), f32),
            vmem((blocks, 5, BLK), f32),
            pltpu.SMEM((1,), f32),
        ),
        in_specs=[pl.BlockSpec(memory_space=pl.ANY)] * len(operands),
        out_specs=(pl.BlockSpec(memory_space=pltpu.VMEM), pl.BlockSpec(memory_space=pltpu.VMEM), pl.BlockSpec(memory_space=pltpu.SMEM)),
        scratch_shapes=[
            pltpu.SMEM(send_list.shape, i32),
            vmem((blocks, 5, BLK), f32),
            vmem((6, blocks, BLK), f32),
            vmem((blocks, 15, BLK), f32),
            vmem((2, padded, BLK), i32),
            vmem((9, padded, BLK), f32),
            vmem((blocks, 20, BLK), f32),
            vmem((n_sub, 20 * capacity, BLK), f32),
            vmem((n_sub, 20 * capacity, BLK), f32),
            vmem((RIM, 5, BLK), f32),
            vmem((RIM, 15, BLK), f32),
            vmem((blocks, 16, BLK), i32),
            vmem((n_sub, capacity, 16, BLK), i32),
            vmem((RIM, 16, BLK), i32),
            vmem((1, BLK), f32),
            vmem((n_dom, n_sub, 1, BLK), f32),
            vmem((n_dom * n_sub, 1, BLK), f32),
            vmem((1, BLK), f32),
            vmem((planes, 1, BLK), f32),
            vmem((n_sub, 5, capacity, BLK), f32),
            vmem((n_sub, 5, capacity, BLK), f32),
            vmem((5, RIM, BLK), f32),
            vmem((5, RIM, BLK), f32),
            vmem((padded, BLK), i32),
            vmem((padded, BLK), i32),
            vmem((padded, BLK), i32),
            vmem((padded, BLK), i32),
            vmem((WORDS, padded, BLK), i32),
            vmem((WORDS, padded, BLK), i32),
            vmem((10, padded, BLK), f32),
            vmem((5 * PIECES, padded, BLK), f32),
            sem((5,)),
            sem,
            sem((2,)),
            sem,
            sem,
            sem,
            sem((2,)),
            sem,
            sem,
            sem,
            sem,
            sem,
            sem,
            pltpu.SemaphoreType.REGULAR,
            pltpu.SemaphoreType.REGULAR,
        ],
        compiler_params=pltpu.CompilerParams(collective_id=0, has_side_effects=True),
        name="hydro_step",
    )(*operands)
    spaces = (pltpu.VMEM, pltpu.VMEM, pltpu.SMEM)
    rate, new, step = (pltpu.with_memory_space_constraint(x, m) for x, m in zip((rate, new, step), spaces))
    rate, new, step = pl.pallas_call(
        finish,
        out_shape=[jax.ShapeDtypeStruct(x.shape, f32) for x in (rate, new, step)],
        in_specs=[pl.BlockSpec(memory_space=space) for space in spaces],
        out_specs=[pl.BlockSpec(memory_space=pl.ANY)] * 3,
        scratch_shapes=[sem((3,))],
        compiler_params=pltpu.CompilerParams(vmem_limit_bytes=2**20),
        name="finish",
    )(rate, new, step)
    flat = lambda x: x.transpose(1, 0, 2).reshape(5, cells)
    return flat(rate), flat(new), step.reshape(())


def solution(mesh):
    both = ("dom", "sub")
    wide, flat = P(None, both), P(both)
    in_specs = (wide, wide, flat, flat, flat, wide, flat, wide, flat, flat, wide, flat, wide, flat)
    out_specs = (wide, wide, P())
    step = functools.partial(body, (mesh.shape["dom"], mesh.shape["sub"]))
    return jax.shard_map(step, mesh=mesh, in_specs=in_specs, out_specs=out_specs, check_vma=False)
```

```python
import functools
import jax
import jax.numpy as jnp
from jax import lax
from jax.experimental import pallas as pl
from jax.experimental.pallas import tpu as pltpu
from jax.sharding import PartitionSpec as P

BLK = 128
RIM = 4
GROUP = 26
PIECES = 2
WORDS = 10
STEPS = 32767.0
PRIM_STEP = 3.0 / STEPS
GRAD_STEP = 1.5 / STEPS

adiabatic = 5.0 / 3.0
courant = 0.3
MESH = pl.DeviceIdType.MESH


def sin_cos(x):
    turns = jnp.floor(x * 0.63661977236 + 0.5)
    r = (x - turns * 1.57079637050628662109375) - turns * -4.37113900018624283e-8
    r2 = r * r
    sine = r + r * r2 * (-1.6666667163e-1 + r2 * (8.3333337680e-3 + r2 * (-1.9841270114e-4 + r2 * 2.7557314297e-6)))
    cosine = 1.0 + r2 * (-0.5 + r2 * (4.1666667908e-2 + r2 * (-1.3888889225e-3 + r2 * 2.4801587642e-5)))
    odd = jnp.abs(turns) == 1.0
    s = jnp.where(odd, cosine, sine)
    c = jnp.where(odd, sine, cosine)
    s = jnp.where((turns < 0.0) | (turns > 1.0), -s, s)
    c = jnp.where((turns > 0.0) | (turns < -1.0), -c, c)
    return s, c


def pack_pair(a, b, scale_a, scale_b):
    high = (a * scale_a + 32768.5).astype(jnp.int32)
    low = (b * scale_b + 32768.5).astype(jnp.int32)
    return lax.shift_left(high, jnp.full_like(high, 16)) + (low + jnp.int32(-(2**31)))


def pack_block(store, upper, lower, rest):
    mixed = lax.broadcasted_iota(jnp.int32, (8, BLK), 0) == 7
    scale = jnp.where(mixed, 1.0 / PRIM_STEP, 1.0 / GRAD_STEP)
    store(0, 8, pack_pair(upper, lower, 1.0 / GRAD_STEP, scale))
    store(8, 2, pack_pair(rest[0:2], rest[2:4], 1.0 / PRIM_STEP, 1.0 / PRIM_STEP))


def side_state(word, offsets):
    high, low = [], []
    for w in range(WORDS):
        value = word(w)
        high.append(lax.shift_right_arithmetic(value, jnp.full_like(value, 16)).astype(jnp.float32))
        low.append(((value & 65535) - 32768).astype(jnp.float32))
    slope = high[:8] + low[:7]
    centre = [low[7], high[8], high[9], low[8], low[9]]
    offsets = [r * GRAD_STEP for r in offsets]
    values = [centre[c] * PRIM_STEP + dot3(slope[3 * c : 3 * c + 3], offsets) for c in range(5)]
    sound = jnp.exp((values[4] - values[0]) * 0.5) * (adiabatic**0.5)
    return jnp.exp(values[0]), values[1:4], jnp.exp(values[4]), sound


def dot3(a, b):
    return a[0] * b[0] + a[1] * b[1] + a[2] * b[2]


def hllc(normal, left, right):
    dl, vl, pl_, cl, ul = left
    dr, vr, pr, cr = right
    ur = dot3(vr, normal)
    signal_l = jnp.minimum(ul - cl, ur - cr)
    signal_r = jnp.maximum(ul + cl, ur + cr)
    mass_l = dl * (signal_l - ul)
    mass_r = dr * (signal_r - ur)
    contact = (pr - pl_ + mass_l * ul - mass_r * ur) / (mass_l - mass_r)
    outer = signal_l >= 0
    from_left = jnp.logical_or(outer, contact >= 0)
    starred = jnp.where(from_left, signal_l, -signal_r) < 0
    pick = lambda a, b: jnp.where(from_left, a, b)
    density, pressure, speed, sound = pick(dl, dr), pick(pl_, pr), pick(ul, ur), pick(cl, cr)
    velocity = [pick(a, b) for a, b in zip(vl, vr)]
    signal, mass_rate = pick(signal_l, signal_r), pick(mass_l, mass_r)
    specific = sound * sound * (1.0 / (adiabatic * (adiabatic - 1.0))) + 0.5 * dot3(velocity, velocity)
    energy = density * specific
    jump = contact - speed
    factor = mass_rate / (signal - contact)
    rise = jnp.where(starred, signal * (factor - density), 0.0)
    push = jnp.where(starred, signal * factor * jump, 0.0)
    rate = density * speed
    out = [rate + rise]
    along = pressure + push
    carry = rate + rise
    for v, n in zip(velocity, normal):
        out.append(carry * v + along * n)
    out.append((energy + pressure) * speed + rise * specific + push * (contact + pressure / mass_rate))
    return out


def lane_gather(row, index):
    table = jnp.broadcast_to(row, index.shape)
    return jnp.take_along_axis(table, index, axis=1, mode="promise_in_bounds")


def flip(index, mask, size):
    out, bit = index, 1
    while bit < size:
        if mask & bit:
            out = out + bit * (1 - 2 * lax.rem(lax.div(index, bit), 2))
        bit *= 2
    return out


def kernel(
    dims,
    send_hbm,
    prim_rows,
    grad_hbm,
    volume_hbm,
    left_hbm,
    right_hbm,
    angles_hbm,
    area_hbm,
    offsets_hbm,
    rim_left_hbm,
    rim_right_hbm,
    rim_angles_hbm,
    rim_area_hbm,
    rim_offsets_hbm,
    rate_out,
    new_out,
    step_out,
    send_list,
    prim,
    cells,
    grad,
    faces,
    shape,
    load_spare,
    outgoing,
    ghosts,
    next_prim,
    next_grad,
    own_packed,
    ghost_packed,
    next_packed,
    min_own,
    mins,
    min_spare,
    min_base,
    ups,
    gback_send,
    gback_recv,
    rback_send,
    rback_recv,
    hi_left,
    lo_left,
    hi_right,
    lo_right,
    left_words,
    right_words,
    ready,
    pieces,
    load_sem,
    ghost_send_sem,
    ghost_recv_sem,
    rim_send_sem,
    rim_recv_sem,
    min_send_sem,
    min_recv_sem,
    up_send_sem,
    up_recv_sem,
    gback_send_sem,
    gback_recv_sem,
    rback_send_sem,
    rback_recv_sem,
    hello,
    hello_next,
):
    n_dom, n_sub, capacity, blocks, face_rows = dims
    rows = face_rows + RIM
    group = max(k for k in range(1, GROUP + 1) if rows % k == 0)
    ghost_blocks = n_sub * capacity
    me_dom = lax.axis_index("dom")
    me_sub = lax.axis_index("sub")
    plane = 1
    planes = n_dom // plane
    my_plane = lax.div(me_dom, plane)
    base_dom = my_plane * plane
    last = me_dom == n_dom - 1
    first = me_dom == 0
    power = n_sub & (n_sub - 1) == 0

    def to_peer(k):
        return flip(me_sub, k, n_sub) if power else lax.rem(me_sub + k, n_sub)

    def from_peer(k):
        return flip(me_sub, k, n_sub) if power else lax.rem(me_sub + n_sub - k, n_sub)

    far_first = list(range(n_sub - 1, 0, -1))
    near = [1]
    parity = lax.rem(me_sub, 2)

    def send_order():
        if not power:
            return [(k, to_peer(k), from_peer(k)) for k in far_first]
        order = []
        for m in range(n_sub - 2, 0, -2):
            even = flip(me_sub, m, n_sub) - parity
            order += [(m + parity, even, even), (m + 1 - parity, even + 1, even + 1)]
        return order + [(1, to_peer(1), from_peer(1))]

    tail = pl.ds(face_rows, RIM)
    body = slice(0, face_rows)
    pairs = [(send_hbm, send_list, 0), (prim_rows, prim, 1)]
    pairs += [(grad_hbm.at[:, h * BLK : (h + 1) * BLK], grad.at[h], 1) for h in range(blocks)]
    pairs += [(prim_rows.at[:, r, :], cells.at[r], 2) for r in range(5)]
    pairs += [(volume_hbm, cells.at[5], 2)]
    middle = len(pairs)
    pairs += [(left_hbm, faces.at[0, body, :], 3), (right_hbm, faces.at[1, body, :], 3)]
    pairs += [(rim_left_hbm, faces.at[0, tail, :], 3), (rim_right_hbm, faces.at[1, tail, :], 3)]
    for where, angle, offset, size in (
        (body, angles_hbm, offsets_hbm, area_hbm),
        (tail, rim_angles_hbm, rim_offsets_hbm, rim_area_hbm),
    ):
        pairs += [(angle.at[:, r, :], shape.at[r, where, :], 4) for r in range(2)]
        pairs += [(offset.at[:, r, :], shape.at[2 + r, where, :], 4) for r in range(6)]
        pairs += [(size, shape.at[8, where, :], 4)]
    loads = [pltpu.make_async_copy(a, b, load_sem.at[k]) for a, b, k in pairs]

    def loaded(k):
        used = slice(0, rows)
        whole = (send_list, load_spare, cells, faces.at[:, used, :], shape.at[:, used, :])[k]
        pltpu.make_async_copy(whole, whole, load_sem.at[k]).wait()

    angles, offsets, area = shape.at[0:2], shape.at[2:8], shape.at[8]
    volume = cells.at[5]
    for load in loads[:middle]:
        load.start()

    barrier = pltpu.get_barrier_semaphore()
    for step in range(plane):
        dom = base_dom + lax.rem(me_dom + step, plane)
        for k in range(n_sub):
            if step or k:
                pl.semaphore_signal(barrier, inc=1, device_id=(dom, to_peer(k)), device_id_type=MESH)

    def greet(p, carry):
        for step in range(plane):
            for k in range(n_sub):
                pl.semaphore_signal(barrier, inc=1, device_id=(p * plane + step, k), device_id_type=MESH)
        return carry

    for load in loads[middle:]:
        load.start()
    lax.fori_loop(my_plane + 1, planes, greet, 0)

    loaded(0)
    loaded(1)
    for k in far_first:
        for j in range(capacity):
            block = jnp.maximum(send_list[to_peer(k) * capacity + j], 0)
            slopes, centres = grad[block], prim[block]
            outgoing[k, 8 * j : 8 * j + 8, :] = slopes[0:8]
            low = 8 * capacity + 8 * j
            outgoing[k, low : low + 7, :] = slopes[8:15]
            outgoing[k, low + 7 : low + 8, :] = centres[0:1]
            outgoing[k, 16 * capacity + 4 * j : 16 * capacity + 4 * j + 4, :] = centres[1:5]

    loaded(2)
    signal = jnp.exp((cells[4] - cells[0]) * 0.5) * (adiabatic**0.5) + jnp.sqrt(
        cells[1] * cells[1] + cells[2] * cells[2] + cells[3] * cells[3]
    )
    limit = jnp.exp(jnp.log(volume[...]) * (1.0 / 3.0)) / signal
    min_own[...] = jnp.min(limit, axis=0, keepdims=True)

    def halves(slopes, centres):
        return slopes[0:8], jnp.concatenate([slopes[8:15], centres[0:1]], 0), centres[1:5]

    for h in range(blocks):

        def store(at, size, value):
            own_packed[h, at : at + size, :] = value

        pack_block(store, *halves(grad[h], prim[h]))

    loaded(3)
    over = pl.ds(face_rows, 8)
    high = lambda x: lax.shift_right_logical(x, jnp.full_like(x, 7))
    for side, hi, lo, shift in ((0, hi_left, lo_left, blocks - RIM), (1, hi_right, lo_right, blocks + ghost_blocks)):
        faces[side, face_rows + RIM : face_rows + 8, :] = faces[side, tail, :]
        hi[body, :] = high(faces[side, body, :])
        lo[...] = faces[side] & (BLK - 1)
        hi[over, :] = high(faces[side, over, :]) + shift

    def row_of(packed):
        return lambda w: packed[w : w + 1, :]

    def gather_into(target, hi, lo, starts, sources, names, keep):
        at = [pl.ds(s, 8) for s in starts]
        index = [lo[here, :] for here in at]
        wanted = [hi[here, :] for here in at]
        match = [[w == name for name in names] for w in wanted]
        for w in range(WORDS):
            values = [target[w, here, :] for here in at] if keep else [None] * len(at)
            for n, row in enumerate(sources):
                line = row(w)
                for i in range(len(at)):
                    got = lane_gather(line, index[i])
                    values[i] = got if values[i] is None else jnp.where(match[i][n], got, values[i])
            for here, value in zip(at, values):
                target[w, here, :] = value

    width = 2 if face_rows % 16 == 0 else 1
    strides = face_rows // (8 * width)

    def gather_main(target, hi, lo, sources, names, keep, begin, end):
        def one(g, carry):
            starts = [pl.multiple_of(g * (8 * width) + 8 * i, 8) for i in range(width)]
            gather_into(target, hi, lo, starts, sources, names, keep)
            return carry

        lax.fori_loop(begin, end, one, 0)

    own = [row_of(own_packed.at[h]) for h in range(blocks)]

    def gather_left(begin, end):
        gather_main(left_words, hi_left, lo_left, own, range(blocks), False, begin, end)

    begun = jnp.where(jnp.logical_and(first, me_sub < 2), max(strides - 1, 0), 0)
    gather_left(0, begun)

    count = plane * n_sub - 1 + plane * n_sub * my_plane
    pl.semaphore_wait(barrier, count)

    def await_all(some, semaphore):
        pltpu.make_async_copy(some, some, semaphore).wait()

    def remote(src, dst, send, recv, dom, sub):
        return pltpu.make_async_remote_copy(
            src_ref=src, dst_ref=dst, send_sem=send, recv_sem=recv, device_id=(dom, sub), device_id_type=MESH
        )

    def min_copy(dom, sub, p):
        here = mins.at[me_dom, me_sub]
        return remote(min_own, here, min_send_sem, min_recv_sem.at[0 if p is None else 1], dom, sub)

    for step in range(plane):
        dom = base_dom + lax.rem(me_dom + step, plane)
        for k in range(n_sub):
            if step or k:
                min_copy(dom, to_peer(k), None).start()

    for k, peer, _ in send_order():
        arrival = ghost_recv_sem.at[0 if isinstance(k, int) and k in near else 1]
        remote(outgoing.at[k], ghosts.at[k], ghost_send_sem, arrival, me_dom, peer).start()
    rim_copies = [
        remote(src.at[0:RIM], dst, rim_send_sem, rim_recv_sem, me_dom - 1, me_sub)
        for src, dst in ((prim, next_prim), (grad, next_grad))
    ]

    def tell(p, carry):
        for step in range(plane):
            for k in range(n_sub):
                min_copy(p * plane + step, k, p).start()
        return carry

    @pl.when(jnp.logical_not(first))
    def _():
        for copy in rim_copies:
            copy.start()

    lax.fori_loop(0, my_plane, tell, 0)

    def hail(p, carry):
        there = (lax.rem(me_dom, plane) + p * plane, me_sub)
        pl.semaphore_signal(hello, inc=1, device_id=there, device_id_type=MESH)
        return carry

    lax.fori_loop(0, my_plane, hail, 0)

    @pl.when(jnp.logical_and(lax.rem(me_dom, plane) == 0, me_dom > 0))
    def _():
        pl.semaphore_signal(hello_next, inc=1, device_id=(me_dom - 1, me_sub), device_id_type=MESH)

    gather_left(begun, strides)
    gather_into(left_words, hi_left, lo_left, [face_rows], own[blocks - RIM :], range(blocks - RIM, blocks), False)

    def pack_ghosts(k):
        for j in range(capacity):
            low, rest = 8 * capacity + 8 * j, 16 * capacity + 4 * j

            def store(at, size, value):
                ghost_packed[k, j, at : at + size, :] = value

            pack_block(
                store, ghosts[k, 8 * j : 8 * j + 8, :], ghosts[k, low : low + 8, :], ghosts[k, rest : rest + 4, :]
            )

    def arrived(ks, semaphore):
        await_all(ghosts.at[min(ks) : max(ks) + 1], semaphore)
        for k in ks:
            pack_ghosts(k)
        lines = [row_of(ghost_packed.at[k, j]) for k in ks for j in range(capacity)]
        return lines, [blocks + from_peer(k) * capacity + j for k in ks for j in range(capacity)]

    more, called = arrived(near, ghost_recv_sem.at[0])
    sources, names = own + more, list(range(blocks)) + called
    gather_main(right_words, hi_right, lo_right, sources, names, False, 0, strides)

    loaded(4)
    for r in range(9):
        shape[r, face_rows + RIM : face_rows + 8, :] = shape[r, tail, :]

    def left_step(g, carry):
        here = pl.ds(pl.multiple_of(g * 8, 8), 8)
        sin_a, cos_a = sin_cos(angles[0, here, :])
        sin_b, cos_b = sin_cos(angles[1, here, :])
        normal = [sin_a * cos_b, sin_a * sin_b, cos_a]
        density, velocity, pressure, sound = side_state(
            lambda w: left_words[w, here, :],
            [offsets[k, here, :] for k in range(3)],
        )
        values = normal + [density] + velocity + [pressure, sound, dot3(velocity, normal)]
        for k, value in enumerate(values):
            ready[k, here, :] = value
        return carry

    lax.fori_loop(0, (face_rows + 8) // 8, left_step, 0)


    def flux_step(g):
        here = pl.ds(g * 8, 8)
        kept = [ready[k, here, :] for k in range(10)]
        right = side_state(
            lambda w: right_words[w, here, :],
            [offsets[k, here, :] for k in range(3, 6)],
        )
        flux = hllc(kept[:3], (kept[3], kept[4:7], kept[7], kept[8], kept[9]), right)
        for c in range(5):
            value = flux[c] * area[here, :]
            if g * 8 >= face_rows:
                value = jnp.where(last, 0.0, value)
            big = value.astype(jnp.bfloat16).astype(jnp.float32)
            pieces[c, here, :] = big
            pieces[5 + c, here, :] = value - big

    lane_iota = lax.broadcasted_iota(jnp.int32, (BLK, BLK), 0)

    def one_hot(lo, s):
        return jnp.where(lane_iota == lo[pl.ds(s, 1), :], 1.0, 0.0).astype(jnp.bfloat16)

    def spread(hi, s, place, sign):
        match = place == hi[pl.ds(s, 1), :]
        parts = []
        for c in range(5 * PIECES):
            value = pieces[c, pl.ds(s, 1), :]
            value = value if sign > 0 else -value
            parts.append(jnp.where(match, value, 0.0))
        return jnp.concatenate(parts, 0).astype(jnp.bfloat16)

    def product(a, b):
        return lax.dot_general(a, b, (((1,), (1,)), ((), ())), preferred_element_type=jnp.float32)

    def fold(total, count):
        total = total.reshape(PIECES, 5, count, BLK)
        return total[0] + total[1]

    sent = (n_sub - 1) * capacity
    away = -(-sent // 8) * 8
    spot = lax.broadcasted_iota(jnp.int32, (away, BLK), 0)
    away_place = jnp.full_like(spot, -1)
    for k in range(1, n_sub):
        lower = (k - 1) * capacity
        away_place = jnp.where(
            (spot >= lower) & (spot < lower + capacity), spot - lower + (blocks + from_peer(k) * capacity), away_place
        )
    own_place = lax.broadcasted_iota(jnp.int32, (blocks, BLK), 0)

    def away_rows(which, place):
        a = jnp.concatenate([spread(hi_right, s, place, -1) for s in which], 1)
        b = jnp.concatenate([one_hot(lo_right, s) for s in which], 1)
        return product(a, b)

    lines, called = arrived([k for k in far_first if k not in near], ghost_recv_sem.at[1])
    total = jnp.zeros((5 * PIECES * away, BLK), jnp.float32)
    span = 8 * width
    for t in range(strides + 2):
        if t < strides:
            at = [t * span + 8 * i for i in range(width)]
            gather_into(right_words, hi_right, lo_right, at, lines, called, True)
        if 1 <= t <= strides:
            for i in range(width):
                flux_step((t - 1) * width + i)
        if t >= 2:
            total = total + away_rows(range((t - 2) * span, (t - 1) * span), away_place)
    total = fold(total, away)
    for k in range(1, n_sub):
        gback_send[k] = total[:, (k - 1) * capacity : k * capacity, :]
    for k, _, peer in send_order():
        remote(gback_send.at[k], gback_recv.at[k], gback_send_sem, gback_recv_sem, me_dom, peer).start()
    @pl.when(last)
    def _():
        next_prim[...] = jnp.zeros_like(next_prim)
        next_grad[...] = jnp.zeros_like(next_grad)

    @pl.when(jnp.logical_not(last))
    def _():
        await_all(load_spare.at[0:RIM], rim_recv_sem)

    for h in range(RIM):
        def store(at, size, value):
            next_packed[h, at : at + size, :] = value

        pack_block(store, *halves(next_grad[h], next_prim[h]))
    def rim_rows():
        start = blocks + ghost_blocks
        gather_into(
            right_words,
            hi_right,
            lo_right,
            [face_rows],
            [row_of(next_packed.at[h]) for h in range(RIM)],
            range(start, start + RIM),
            False,
        )


    rim_rows()
    flux_step(face_rows // 8)
    rim_place = lax.broadcasted_iota(jnp.int32, (8, BLK), 0) + (blocks + ghost_blocks)
    total = fold(away_rows(range(face_rows, rows), rim_place), 8)
    rback_send[...] = total[:, 0:RIM, :]
    rback_copy = remote(rback_send, rback_recv, rback_send_sem, rback_recv_sem, me_dom + 1, me_sub)

    @pl.when(jnp.logical_and(lax.rem(me_dom, plane) == plane - 1, jnp.logical_not(last)))
    def _():
        pl.semaphore_wait(hello_next, 1)

    @pl.when(jnp.logical_not(last))
    def _():
        rback_copy.start()

    def await_mins(semaphore, count):
        for p in range(planes):
            if count(p) > 0:

                @pl.when(my_plane == p)
                def _():
                    await_all(min_spare.at[0 : count(p)], semaphore)

    def up_copy(p):
        there = lax.rem(me_dom, plane) + p * plane
        return remote(min_base, ups.at[my_plane], up_send_sem, up_recv_sem, there, me_sub)

    def tell_later():
        await_all(min_spare.at[0 : plane * n_sub - 1], min_recv_sem.at[0])
        small = min_own[...]
        for step in range(1, plane * n_sub):
            dom = base_dom + lax.rem(me_dom + step // n_sub, plane)
            sub = lax.rem(me_sub + step, n_sub)
            small = jnp.minimum(small, mins[dom, sub])
        min_base[...] = small

        @pl.when(my_plane < planes - 1)
        def _():
            pl.semaphore_wait(hello, planes - 1 - my_plane)

        def one(p, carry):
            up_copy(p).start()
            return carry

        lax.fori_loop(my_plane + 1, planes, one, 0)

    tell_later()

    def local_step(i, total):
        a = [spread(hi_left, i * group + k, own_place, 1) for k in range(group)]
        a += [spread(hi_right, i * group + k, own_place, -1) for k in range(group)]
        b = [one_hot(lo_left, i * group + k) for k in range(group)]
        b += [one_hot(lo_right, i * group + k) for k in range(group)]
        return total + product(jnp.concatenate(a, 1), jnp.concatenate(b, 1))

    total = lax.fori_loop(0, rows // group, local_step, jnp.zeros((5 * PIECES * blocks, BLK), jnp.float32))
    net = fold(total, blocks)

    await_mins(up_recv_sem, lambda p: p)
    await_mins(min_recv_sem.at[1], lambda p: plane * n_sub * (planes - 1 - p))

    def earlier(p, small):
        return jnp.minimum(small, ups[p])

    smallest = lax.fori_loop(0, my_plane, earlier, min_base[...])

    def later(p, small):
        for step in range(plane):
            for k in range(n_sub):
                small = jnp.minimum(small, mins[p * plane + step, k])
        return small

    smallest = lax.fori_loop(my_plane + 1, planes, later, smallest)
    time_step = courant * jnp.min(smallest, axis=1, keepdims=True)
    step_out[0] = courant * jnp.min(smallest)

    @pl.when(first)
    def _():
        rback_recv[...] = jnp.zeros_like(rback_recv)

    @pl.when(jnp.logical_not(first))
    def _():
        rback_copy.wait_recv()

    await_all(gback_recv.at[1:n_sub], gback_recv_sem)

    square = cells[1] * cells[1] + cells[2] * cells[2] + cells[3] * cells[3]
    density = jnp.exp(cells[0])
    energy = jnp.exp(cells[4]) / (adiabatic - 1.0) + 0.5 * density * square
    conserved = [density, density * cells[1], density * cells[2], density * cells[3], energy]
    inverse = -1.0 / volume[...]
    for c in range(5):
        sums = net[c]
        for h in range(RIM):
            sums = sums + jnp.where(own_place == h, rback_recv[c, h : h + 1, :], 0.0)
        for k in range(1, n_sub):
            for j in range(capacity):
                wanted = send_list[to_peer(k) * capacity + j]
                sums = sums + jnp.where(own_place == wanted, gback_recv[k, c, j : j + 1, :], 0.0)
        rate = sums * inverse
        new = conserved[c] + time_step * rate
        rate_out[:, c, :] = rate
        new_out[:, c, :] = new

    @pl.when(jnp.logical_not(first))
    def _():
        await_all(load_spare.at[0:RIM], rim_send_sem)

    @pl.when(jnp.logical_not(last))
    def _():
        rback_copy.wait_send()

    await_all(ghosts.at[1:n_sub], ghost_send_sem)
    await_all(gback_recv.at[1:n_sub], gback_send_sem)
    await_mins(min_send_sem, lambda p: plane * n_sub * (p + 1) - 1)
    await_mins(up_send_sem, lambda p: planes - 1 - p)


def finish(rate, new, step, rate_out, new_out, step_out, sems):
    pairs = ((rate, rate_out), (new, new_out), (step, step_out))
    copies = [pltpu.make_async_copy(a, b, sems.at[k]) for k, (a, b) in enumerate(pairs)]
    for copy in copies:
        copy.start()
    for copy in copies:
        copy.wait()


def by_block(x):
    return x.reshape(x.shape[0], x.shape[1] // BLK, BLK).transpose(1, 0, 2)


def body(mesh_sizes, *args):
    (primitive, gradient, volume, face_left, face_right, face_angles, face_area, face_offsets) = args[:8]
    (rim_left, rim_right, rim_angles, rim_area, rim_offsets, send_list) = args[8:]
    n_dom, n_sub = mesh_sizes
    cells = primitive.shape[1]
    blocks = cells // BLK
    face_rows = face_left.shape[0] // BLK
    capacity = send_list.shape[0] // n_sub
    padded = face_rows + 8
    dims = (n_dom, n_sub, capacity, blocks, face_rows)
    f32, i32 = jnp.float32, jnp.int32
    planes = n_dom
    sem = pltpu.SemaphoreType.DMA
    operands = (
        send_list,
        by_block(primitive),
        gradient,
        volume.reshape(blocks, BLK),
        face_left.reshape(face_rows, BLK),
        face_right.reshape(face_rows, BLK),
        by_block(face_angles),
        face_area.reshape(face_rows, BLK),
        by_block(face_offsets),
        rim_left.reshape(RIM, BLK),
        rim_right.reshape(RIM, BLK),
        by_block(rim_angles),
        rim_area.reshape(RIM, BLK),
        by_block(rim_offsets),
    )
    vmem = pltpu.VMEM
    rate, new, step = pl.pallas_call(
        functools.partial(kernel, dims),
        out_shape=(
            vmem((blocks, 5, BLK), f32),
            vmem((blocks, 5, BLK), f32),
            pltpu.SMEM((1,), f32),
        ),
        in_specs=[pl.BlockSpec(memory_space=pl.ANY)] * len(operands),
        out_specs=(pl.BlockSpec(memory_space=pltpu.VMEM), pl.BlockSpec(memory_space=pltpu.VMEM), pl.BlockSpec(memory_space=pltpu.SMEM)),
        scratch_shapes=[
            pltpu.SMEM(send_list.shape, i32),
            vmem((blocks, 5, BLK), f32),
            vmem((6, blocks, BLK), f32),
            vmem((blocks, 15, BLK), f32),
            vmem((2, padded, BLK), i32),
            vmem((9, padded, BLK), f32),
            vmem((blocks, 20, BLK), f32),
            vmem((n_sub, 20 * capacity, BLK), f32),
            vmem((n_sub, 20 * capacity, BLK), f32),
            vmem((RIM, 5, BLK), f32),
            vmem((RIM, 15, BLK), f32),
            vmem((blocks, 16, BLK), i32),
            vmem((n_sub, capacity, 16, BLK), i32),
            vmem((RIM, 16, BLK), i32),
            vmem((1, BLK), f32),
            vmem((n_dom, n_sub, 1, BLK), f32),
            vmem((n_dom * n_sub, 1, BLK), f32),
            vmem((1, BLK), f32),
            vmem((planes, 1, BLK), f32),
            vmem((n_sub, 5, capacity, BLK), f32),
            vmem((n_sub, 5, capacity, BLK), f32),
            vmem((5, RIM, BLK), f32),
            vmem((5, RIM, BLK), f32),
            vmem((padded, BLK), i32),
            vmem((padded, BLK), i32),
            vmem((padded, BLK), i32),
            vmem((padded, BLK), i32),
            vmem((WORDS, padded, BLK), i32),
            vmem((WORDS, padded, BLK), i32),
            vmem((10, padded, BLK), f32),
            vmem((5 * PIECES, padded, BLK), f32),
            sem((5,)),
            sem,
            sem((2,)),
            sem,
            sem,
            sem,
            sem((2,)),
            sem,
            sem,
            sem,
            sem,
            sem,
            sem,
            pltpu.SemaphoreType.REGULAR,
            pltpu.SemaphoreType.REGULAR,
        ],
        compiler_params=pltpu.CompilerParams(collective_id=0, has_side_effects=True),
        name="hydro_step",
    )(*operands)
    spaces = (pltpu.VMEM, pltpu.VMEM, pltpu.SMEM)
    rate, new, step = (pltpu.with_memory_space_constraint(x, m) for x, m in zip((rate, new, step), spaces))
    rate, new, step = pl.pallas_call(
        finish,
        out_shape=[jax.ShapeDtypeStruct(x.shape, f32) for x in (rate, new, step)],
        in_specs=[pl.BlockSpec(memory_space=space) for space in spaces],
        out_specs=[pl.BlockSpec(memory_space=pl.ANY)] * 3,
        scratch_shapes=[sem((3,))],
        compiler_params=pltpu.CompilerParams(vmem_limit_bytes=2**20),
        name="finish",
    )(rate, new, step)
    flat = lambda x: x.transpose(1, 0, 2).reshape(5, cells)
    return flat(rate), flat(new), step.reshape(())


def solution(mesh):
    both = ("dom", "sub")
    wide, flat = P(None, both), P(both)
    in_specs = (wide, wide, flat, flat, flat, wide, flat, wide, flat, flat, wide, flat, wide, flat)
    out_specs = (wide, wide, P())
    step = functools.partial(body, (mesh.shape["dom"], mesh.shape["sub"]))
    return jax.shard_map(step, mesh=mesh, in_specs=in_specs, out_specs=out_specs, check_vma=False)
```
